256 devices in a mesh: wide: 16 (over x, y), grp: 16 (over z, core).
Axes of the slice: x: 4, y: 4, z: 8, core: 2. Of those that a mesh axis runs over, the one named last changes fastest.
Arguments:
- surf_depth: int32 [16, 16, 16, 4096], P('wide', 'grp'), may hold values from 0 to 1073741823
- surf_color: bfloat16 [16, 16, 16, 3, 4096], P('wide', 'grp'), may hold values from 0 to 2
- surf_box: int32 [16, 16, 16, 4], P('wide', 'grp'), may hold values from 0 to 64, as said below
- vol_color: bfloat16 [16, 16, 16, 8, 3, 4096], P('wide', 'grp'), may hold values from 0 to 4
- vol_alpha: bfloat16 [16, 16, 16, 8, 4096], P('wide', 'grp'), may hold values from 0.0009994507 to 0.039794922
- vol_box: int32 [16, 16, 16, 4], P('wide', 'grp'), may hold values from 0 to 64, as said below
- ray_entry: int32 [16, 16, 16, 4096], P('wide', 'grp'), may hold values from 0 to 939524095
- ray_step: int32 [16, 16, 16, 4096], P('wide', 'grp'), may hold values from 1048576 to 16777215
- order: int32 [16, 16], P('grp'), may hold values from 0 to 15, each once within a row
Outputs:
- frame: float32 [16, 16, 4, 4096], P('grp', 'wide')
The draws below stay inside these ranges and needn't reach their ends.
Inputs may be any that keep to these rules, and one draw needn't show every extreme that they name: `surf_box`: each box gives rows [top, bottom) and columns [left, right) of a tile with 1 to 16 rows and 1 or more columns; in every draw one tile row has boxes of exactly 16 rows from every source, and other tiles reach it too. `vol_box`: each box gives rows [top, bottom) and columns [left, right) of a tile with 1 to 32 rows and 1 or more columns; in every draw one tile column has boxes of exactly 32 rows from every brick of every band, and other tiles reach it too. `order`: each row is a permutation of 0 .. 15.
All inputs are finite; a program needn't handle non-finite values.
Results may differ from the reference program's by a relative error of at most 0.0003.
Values may be sent and summed in bfloat16 or wider, within the bound.
A program may use at most 64 MiB of HBM per device.

```python
import math
import jax
import jax.numpy as jnp
from jax import lax

TILE_H = 64
TILE_W = 64
TPIX = 4096
SAMPLES = 8
SBOX_ROWS = 16
VBOX_ROWS = 32
N_WIDE = 16
N_GRP = 16


def draw_boxes(key, lead, most, full_axis):
    keys = jax.random.split(key, 6)
    height = jax.random.randint(keys[0], lead, 1, most + 1)
    force = jax.random.randint(keys[1], lead, 0, 4) == 0
    chosen = jax.random.randint(keys[2], (), 0, lead[full_axis])
    position = lax.broadcasted_iota(jnp.int32, lead, full_axis)
    height = jnp.where(force | (position == chosen), most, height)
    top = jax.random.randint(keys[3], lead, 0, TILE_H - height + 1)
    width = jax.random.randint(keys[4], lead, 1, TILE_W + 1)
    left = jax.random.randint(keys[5], lead, 0, TILE_W - width + 1)
    return jnp.stack([top, top + height, left, left + width], axis=-1).astype(jnp.int32)


def draw_surf_box(key, part):
    return draw_boxes(jax.random.fold_in(key, 11), (N_WIDE, N_GRP, N_GRP), SBOX_ROWS, 2)


def draw_vol_box(key, part):
    return draw_boxes(jax.random.fold_in(key, 23), (N_WIDE, N_GRP, N_WIDE), VBOX_ROWS, 2)


def plant(entries, rng, smallest, largest):
    extent = entries.shape
    spot = [jax.random.randint(jax.random.fold_in(rng, axis), (), 0, extent[axis]) for axis in range(len(extent))]
    entries = entries.at[tuple(spot)].set(smallest)
    longest = extent.index(max(extent))
    spot[longest] = (spot[longest] + 1) % extent[longest]
    return entries.at[tuple(spot)].set(largest)


def levels(own_key, extent, pieces, smallest, high):
    factor_of = 1.0
    for dim, shards_of in pieces:
        steps = jax.random.uniform(jax.random.fold_in(jax.random.fold_in(own_key, 6), dim), (shards_of,), jnp.float32, smallest / len(pieces), high / len(pieces))
        factor_of = factor_of * jnp.repeat(jnp.exp(steps), extent[dim] // shards_of).reshape((-1,) + (1,) * (len(extent) - 1 - dim))
    return factor_of


def setup_inputs(seed: int = 0) -> dict:
    arg_keys = jax.random.split(jax.random.key(seed), 10)
    surf_depth = plant(jax.random.randint(arg_keys[0], (N_WIDE, N_GRP, N_GRP, TPIX), 0, 1073741824), jax.random.fold_in(arg_keys[0], 1), 0, 1073741823).astype(jnp.int32)
    surf_color = jnp.clip(2.0 * jax.random.uniform(arg_keys[1], (N_WIDE, N_GRP, N_GRP, 3, TPIX), jnp.float32) ** levels(arg_keys[1], (N_WIDE, N_GRP, N_GRP, 3, TPIX), ((0, 16), (1, 16)), -0.2, 0.2), 0.0, 2.0).astype(jnp.bfloat16)
    surf_box = draw_surf_box(jax.random.fold_in(arg_keys[9], 71), 0)
    vol_color = jnp.clip(4.0 * jax.random.uniform(arg_keys[3], (N_WIDE, N_GRP, N_WIDE, SAMPLES, 3, TPIX), jnp.float32) ** levels(arg_keys[3], (N_WIDE, N_GRP, N_WIDE, SAMPLES, 3, TPIX), ((0, 16), (1, 16)), -0.2, 0.2), 0.0, 4.0).astype(jnp.bfloat16)
    vol_alpha = jnp.clip(jnp.exp(math.log(0.039794922) - 3.6842888 * jax.random.uniform(arg_keys[4], (N_WIDE, N_GRP, N_WIDE, SAMPLES, TPIX), jnp.float32) ** levels(arg_keys[4], (N_WIDE, N_GRP, N_WIDE, SAMPLES, TPIX), ((0, 16), (1, 16)), -0.2, 0.2)), 0.0009994507, 0.039794922).astype(jnp.bfloat16)
    vol_box = draw_vol_box(jax.random.fold_in(arg_keys[9], 71), 0)
    ray_entry = plant(jax.random.randint(arg_keys[6], (N_WIDE, N_GRP, N_WIDE, TPIX), 0, 939524096), jax.random.fold_in(arg_keys[6], 1), 0, 939524095).astype(jnp.int32)
    ray_step = plant(jax.random.randint(arg_keys[7], (N_WIDE, N_GRP, N_WIDE, TPIX), 1048576, 16777216), jax.random.fold_in(arg_keys[7], 1), 1048576, 16777215).astype(jnp.int32)
    order = jax.vmap(lambda own: jax.random.permutation(own, N_WIDE))(jax.random.split(arg_keys[8], N_GRP)).reshape((N_GRP, N_WIDE)).astype(jnp.int32)
    return dict(surf_depth=surf_depth, surf_color=surf_color, surf_box=surf_box, vol_color=vol_color, vol_alpha=vol_alpha, vol_box=vol_box, ray_entry=ray_entry, ray_step=ray_step, order=order)


far_depth = 1073741824


def window_mask(box, start, rows, tile_w):
    row_ids = start[..., None, None] + jnp.arange(rows, dtype=jnp.int32)[:, None]
    col_ids = jnp.arange(tile_w, dtype=jnp.int32)[None, :]
    inside = (row_ids >= box[..., 0, None, None]) & (row_ids < box[..., 1, None, None])
    inside = inside & (col_ids >= box[..., 2, None, None]) & (col_ids < box[..., 3, None, None])
    return inside.reshape(box.shape[:-1] + (rows * tile_w,))


def integrate(color, alpha, inside, entry, stride, limit):
    accum = jnp.zeros(alpha.shape[:-2] + (3, alpha.shape[-1]), jnp.float32)
    trans = jnp.ones(alpha.shape[:-2] + (alpha.shape[-1],), jnp.float32)
    for k in range(SAMPLES):
        kept = inside & (entry + k * stride < limit)
        opacity = alpha[..., k, :].astype(jnp.float32)
        weight = jnp.where(kept, trans * opacity, 0.0)
        accum = accum + weight[..., None, :] * color[..., k, :, :].astype(jnp.float32)
        trans = trans * (1.0 - jnp.where(kept, opacity, 0.0))
    return accum, trans


def reference(surf_depth, surf_color, surf_box, vol_color, vol_alpha, vol_box, ray_entry, ray_step, order):
    present = window_mask(surf_box, jnp.zeros(surf_box.shape[:-1], jnp.int32), TILE_H, TILE_W)
    frag_depth = jnp.where(present, surf_depth, far_depth)
    nearest = jnp.min(frag_depth, axis=1)
    winner = jnp.argmin(frag_depth, axis=1).astype(jnp.int32)
    sources = jnp.arange(N_GRP, dtype=jnp.int32)[None, :, None, None]
    pick = (sources == winner[:, None]) & present
    surface = jnp.sum(jnp.where(pick[:, :, :, None, :], surf_color.astype(jnp.float32), 0.0), axis=1)

    def one_band(band):
        color = lax.dynamic_index_in_dim(vol_color, band, 1, keepdims=False)
        alpha = lax.dynamic_index_in_dim(vol_alpha, band, 1, keepdims=False)
        box = lax.dynamic_index_in_dim(vol_box, band, 1, keepdims=False)
        entry = lax.dynamic_index_in_dim(ray_entry, band, 1, keepdims=False)
        stride = lax.dynamic_index_in_dim(ray_step, band, 1, keepdims=False)
        limit = lax.dynamic_index_in_dim(nearest, band, 1, keepdims=False)
        inside = window_mask(box, jnp.zeros(box.shape[:-1], jnp.int32), TILE_H, TILE_W)
        accum, trans = integrate(color, alpha, inside, entry, stride, limit[None])
        rank = lax.dynamic_index_in_dim(order, band, 0, keepdims=False)
        ordered_accum = jnp.take(accum, rank, axis=0)
        ordered_trans = jnp.take(trans, rank, axis=0)

        def over(carry, layer):
            color_sum, through = carry
            return (color_sum + through[:, None, :] * layer[0], through * layer[1]), None

        start = (jnp.zeros(accum.shape[1:], jnp.float32), jnp.ones(trans.shape[1:], jnp.float32))
        (color_sum, through), unused = lax.scan(over, start, (ordered_accum, ordered_trans))
        behind = lax.dynamic_index_in_dim(surface, band, 1, keepdims=False)
        rgb = color_sum + through[:, None, :] * behind
        return jnp.concatenate([rgb, through[:, None, :]], axis=1)

    return lax.map(one_band, jnp.arange(N_GRP, dtype=jnp.int32))
```

```python
import functools

import jax
import jax.numpy as jnp
from jax import lax
from jax.experimental import pallas as pl
from jax.experimental.pallas import tpu as pltpu
from jax.sharding import PartitionSpec as P

MESH = pl.DeviceIdType.MESH
FAR = 1073741824
PIX = 4096
LROWS = 32
S = 40
SAMPLES = 8
COLOR_SCALE = 59000.0
ALPHA_SCALE = 236000.0

I32 = jnp.int32
F32 = jnp.float32


def far_first(nx, ny):
    ring = lambda d, n: min(d, n - d)
    offsets = [(a, b) for a in range(nx) for b in range(ny) if (a, b) != (0, 0)]
    return sorted(offsets, key=lambda o: -(ring(o[0], nx) + ring(o[1], ny)))


def kernel(
    dims,
    sdepth, scolor, sbox, vcolor, valpha, vbox, entry, step, order,
    out,
    sd_nat, sc_nat, vc_nat, va_nat, en_nat, st_nat,
    sd, sc, en, st, ad, cd,
    a_send, a_recv, c_send, c_recv, t_send, t_recv, l_send, l_recv, f_send, f_recv,
    tab0, tab1, surf, od,
    lsem, a_ss, a_rs, c_ss, c_rs, t_ss, t_rs, l_ss, l_rs, f_ss, f_rs,
):
    nx, ny, nz, ncore = dims
    nw, ng = nx * ny, nz * ncore
    me_w, me_g = lax.axis_index("wide"), lax.axis_index("grp")
    wide_offsets, grp_offsets = far_first(nx, ny), far_first(nz, ncore)

    def wide_peer(o):
        x, y = me_w // ny, me_w % ny
        return ((x + o[0]) % nx) * ny + (y + o[1]) % ny

    def grp_peer(o):
        z, core = me_g // ncore, me_g % ncore
        return ((z + o[0]) % nz) * ncore + (core + o[1]) % ncore

    def wide_copy(o, src, dst, ss, rs):
        peer = wide_peer(o)
        return pltpu.make_async_remote_copy(
            src_ref=src.at[peer], dst_ref=dst.at[me_w], send_sem=ss.at[peer], recv_sem=rs.at[me_w],
            device_id=(peer, me_g), device_id_type=MESH,
        )

    def grp_copy(o, src, dst, ss, rs):
        peer = grp_peer(o)
        return pltpu.make_async_remote_copy(
            src_ref=src.at[peer], dst_ref=dst.at[me_g], send_sem=ss.at[peer], recv_sem=rs.at[me_g],
            device_id=(me_w, peer), device_id_type=MESH,
        )

    def arrived(peer, buf, rs):
        pltpu.make_async_copy(buf.at[peer], buf.at[peer], rs.at[peer]).wait()

    def left(peer, buf, ss):
        pltpu.make_async_copy(buf.at[peer], buf.at[peer], ss.at[peer]).wait()

    loads = []
    for i, (src, dst) in enumerate(
        ((sdepth, sd_nat), (valpha, va_nat), (vcolor, vc_nat), (entry, en_nat), (step, st_nat), (scolor, sc_nat))
    ):
        loads.append(pltpu.make_async_copy(src, dst, lsem.at[i]))
        loads[-1].start()

    barrier = pltpu.get_barrier_semaphore()
    for o in grp_offsets:
        pl.semaphore_signal(barrier, inc=1, device_id=(me_w, grp_peer(o)), device_id_type=MESH)
    for o in wide_offsets:
        pl.semaphore_signal(barrier, inc=1, device_id=(wide_peer(o), me_g), device_id_type=MESH)

    row8 = lax.broadcasted_iota(I32, (8, 128), 0)
    lane8 = lax.broadcasted_iota(I32, (8, 128), 1)
    fold8 = 2 * row8 + (lane8 >> 6)
    col8 = lane8 & 63
    fold16 = 2 * lax.broadcasted_iota(I32, (16, 128), 0) + (lax.broadcasted_iota(I32, (16, 128), 1) >> 6)
    col16 = lax.broadcasted_iota(I32, (16, 128), 1) & 63

    def spread(nat, dense, n, lead=()):
        g = min(8, n)
        for h in range(n // g):
            for j in range(LROWS):
                tile = nat[(*lead, pl.ds(h * g, g), pl.ds(128 * j, 128))]
                if tile.dtype == jnp.bfloat16:
                    tile = tile.astype(F32)
                dense[pl.ds(h * g * S + j, g, stride=S), :] = tile

    loads[0].wait()
    spread(sd_nat, sd, ng)

    def surface_inside(r):
        inx = (col8 >= sbox[2, r]) & (col8 < sbox[3, r])
        return [
            inx & (fold8 + 16 * q >= sbox[0, r]) & (fold8 + 16 * q < sbox[1, r]) for q in range(4)
        ]

    for r in range(ng):
        folded = jnp.full((8, 128), FAR, I32)
        for q, inside in enumerate(surface_inside(r)):
            folded = jnp.where(inside, sd[pl.ds(r * S + 8 * q, 8), :], folded)
        a_send[r, 0:8, :] = folded
        a_send[r, 8:9, :] = jnp.full((1, 128), sbox[0, r], I32)
    for c in range(nw):
        t_send[c] = jnp.full((1, 128), vbox[0, c], I32)
    a_recv[me_g] = a_send[me_g]
    t_recv[me_w] = t_send[me_w]

    pl.semaphore_wait(barrier, nw + ng - 2)
    for o in grp_offsets:
        grp_copy(o, a_send, a_recv, a_ss, a_rs).start()
    for o in wide_offsets:
        wide_copy(o, t_send, t_recv, t_ss, t_rs).start()

    loads[5].wait()
    for ch in range(3):
        spread(sc_nat, sc.at[ch], ng, (ch,))

    def fold_color(r, carry):
        inside = surface_inside(r)
        for ch in range(3):
            folded = jnp.zeros((8, 128), F32)
            for q in range(4):
                folded = jnp.where(inside[q], sc[ch, pl.ds(r * S + 8 * q, 8), :], folded)
            c_send[r, ch] = folded.astype(jnp.bfloat16)
        return carry

    lax.fori_loop(0, ng, fold_color, 0)
    c_recv[me_g] = c_send[me_g]

    for i in (1, 2, 3, 4):
        loads[i].wait()
    spread(en_nat, en, nw)
    spread(st_nat, st, nw)

    lane1 = lax.broadcasted_iota(I32, (8, 128), 1) >> 6

    def prefixes(c, carry):
        top, bottom = vbox[0, c], vbox[1, c]
        for j in range(16):
            s = lane1 + 2 * j
            upper = (top + ((s - top) & 31)) >= 32
            px, px2 = pl.ds(128 * j, 128), pl.ds(128 * (j + 16), 128)
            ad[pl.ds(j, SAMPLES, stride=S), :] = jnp.where(
                upper, va_nat[c, :, px2].astype(F32), va_nat[c, :, px].astype(F32)
            )
            for ch in range(3):
                cd[ch, pl.ds(j, SAMPLES, stride=S), :] = jnp.where(
                    upper, vc_nat[c, ch, :, px2].astype(F32), vc_nat[c, ch, :, px].astype(F32)
                )
        y = top + ((fold16 - top) & 31)
        upper = y >= 32
        inside = (y < bottom) & (col16 >= vbox[2, c]) & (col16 < vbox[3, c])
        first = jnp.where(upper, en[pl.ds(c * S + 16, 16), :], en[pl.ds(c * S, 16), :])
        en[pl.ds(c * S, 16), :] = jnp.where(inside, first, FAR)
        st[pl.ds(c * S, 16), :] = jnp.where(upper, st[pl.ds(c * S + 16, 16), :], st[pl.ds(c * S, 16), :])
        trans = jnp.ones((16, 128), F32)
        accum = [jnp.zeros((16, 128), F32) for _ in range(3)]
        for k in range(SAMPLES):
            alpha = ad[pl.ds(k * S, 16), :]
            weight = trans * alpha
            trans = trans * (1.0 - alpha)
            for ch in range(3):
                accum[ch] = accum[ch] + weight * cd[ch, pl.ds(k * S, 16), :]
            r, g, b = [(a * COLOR_SCALE + 0.5).astype(I32) for a in accum]
            t = ((1.0 - trans) * ALPHA_SCALE + 0.5).astype(I32)
            tab0[c, k] = (r << 16) | g
            tab1[c, k] = (b << 16) | t
        return carry

    lax.fori_loop(0, nw // 2, prefixes, 0)

    for o in reversed(grp_offsets):
        arrived(grp_peer(o), a_recv, a_rs)
    near = [jnp.full((8, 128), FAR, I32) for _ in range(4)]
    winner = [jnp.full((8, 128), -1, I32) for _ in range(4)]
    for s in range(ng):
        depth = a_recv[s, 0:8, :]
        top = a_recv[s, 8:9, :]
        where_q = (top + ((fold8 - top) & 15)) >> 4
        for q in range(4):
            take = (where_q == q) & (depth < near[q])
            near[q] = jnp.where(take, depth, near[q])
            winner[q] = jnp.where(take, s, winner[q])

    for o in reversed(wide_offsets):
        arrived(wide_peer(o), t_recv, t_rs)

    def upper_half(top):
        return (top + ((fold16 - top) & 31)) >= 32

    near_lo = jnp.concatenate(near[:2], axis=0)
    near_hi = jnp.concatenate(near[2:], axis=0)
    for b in range(nw):
        l_send[b] = jnp.where(upper_half(t_recv[b]), near_hi, near_lo)
    l_recv[me_w] = l_send[me_w]
    for o in wide_offsets:
        wide_copy(o, l_send, l_recv, l_ss, l_rs).start()
    for o in grp_offsets:
        grp_copy(o, c_send, c_recv, c_ss, c_rs).start()

    lax.fori_loop(nw // 2, nw, prefixes, 0)

    waiting = None
    for o in [(0, 0), *reversed(wide_offsets)]:
        c = wide_peer(o)
        if o != (0, 0):
            arrived(c, l_recv, l_rs)
        limit = l_recv[c]
        at = en[pl.ds(c * S, 16), :]
        stride = st[pl.ds(c * S, 16), :]
        word0 = jnp.zeros((16, 128), I32)
        word1 = jnp.zeros((16, 128), I32)
        for k in range(SAMPLES):
            kept = at < limit
            word0 = jnp.where(kept, tab0[c, k], word0)
            word1 = jnp.where(kept, tab1[c, k], word1)
            at = at + stride
        if o == (0, 0):
            f_recv[me_w, 0:16, :] = word0
            f_recv[me_w, 16:32, :] = word1
        else:
            f_send[c, 0:16, :] = word0
            f_send[c, 16:32, :] = word1
            if waiting is not None:
                wide_copy(waiting, f_send, f_recv, f_ss, f_rs).start()
            waiting = o
    for o in reversed(grp_offsets):
        arrived(grp_peer(o), c_recv, c_rs)
    wide_copy(waiting, f_send, f_recv, f_ss, f_rs).start()
    color = [[jnp.zeros((8, 128), F32) for _ in range(3)] for _ in range(4)]
    for s in range(ng):
        rgb = [c_recv[s, ch].astype(F32) for ch in range(3)]
        for q in range(4):
            won = winner[q] == s
            color[q] = [jnp.where(won, rgb[ch], color[q][ch]) for ch in range(3)]
    for ch in range(3):
        for q in range(4):
            surf[ch, 8 * q : 8 * q + 8, :] = color[q][ch]

    for o in reversed(wide_offsets):
        arrived(wide_peer(o), f_recv, f_rs)
    through = [jnp.ones((16, 128), F32) for _ in range(2)]
    total = [[jnp.zeros((16, 128), F32) for _ in range(3)] for _ in range(2)]
    for j in range(nw):
        b = order[0, j]
        word0, word1 = f_recv[b, 0:16, :], f_recv[b, 16:32, :]
        upper = upper_half(t_recv[b])
        layer = [
            lax.shift_right_logical(word0, 16).astype(F32),
            (word0 & 65535).astype(F32),
            lax.shift_right_logical(word1, 16).astype(F32),
        ]
        opaque = (word1 & 65535).astype(F32) * (1.0 / ALPHA_SCALE)
        for h in range(2):
            weight = jnp.where(upper, through[h], 0.0) if h else jnp.where(upper, 0.0, through[h])
            total[h] = [total[h][ch] + weight * layer[ch] for ch in range(3)]
            through[h] = through[h] - weight * opaque
    for h in range(2):
        rows = slice(16 * h, 16 * h + 16)
        for ch in range(3):
            od[ch * S + 16 * h : ch * S + 16 * h + 16, :] = (
                total[h][ch] * (1.0 / COLOR_SCALE) + through[h] * surf[ch, rows, :]
            )
        od[3 * S + 16 * h : 3 * S + 16 * h + 16, :] = through[h]
    for j in range(LROWS):
        out[:, 128 * j : 128 * j + 128] = od[pl.ds(j, 4, stride=S), :]

    for o in grp_offsets:
        left(grp_peer(o), a_send, a_ss)
        left(grp_peer(o), c_send, c_ss)
    for o in wide_offsets:
        left(wide_peer(o), t_send, t_ss)
        left(wide_peer(o), l_send, l_ss)
        left(wide_peer(o), f_send, f_ss)


def per_device(dims, surf_depth, surf_color, surf_box, vol_color, vol_alpha, vol_box, ray_entry, ray_step, order):
    nx, ny, nz, ncore = dims
    nw, ng = nx * ny, nz * ncore
    V, D = pltpu.VMEM, pltpu.SemaphoreType.DMA
    bf16 = jnp.bfloat16
    hbm = pl.BlockSpec(memory_space=pltpu.HBM)
    smem = pl.BlockSpec(memory_space=pltpu.SMEM)
    frame = pl.pallas_call(
        functools.partial(kernel, dims),
        out_shape=jax.ShapeDtypeStruct((4, PIX), F32),
        in_specs=[hbm, hbm, smem, hbm, hbm, smem, hbm, hbm, smem],
        out_specs=pl.BlockSpec(memory_space=pltpu.VMEM),
        scratch_shapes=[
            V((ng, PIX), I32), V((3, ng, PIX), bf16), V((nw, 3, SAMPLES, PIX), bf16), V((nw, SAMPLES, PIX), bf16),
            V((nw, PIX), I32), V((nw, PIX), I32),
            V((ng * S, 128), I32), V((3, ng * S, 128), F32), V((nw * S, 128), I32), V((nw * S, 128), I32),
            V((SAMPLES * S, 128), F32), V((3, SAMPLES * S, 128), F32),
            V((ng, 9, 128), I32), V((ng, 9, 128), I32),
            V((ng, 3, 8, 128), bf16), V((ng, 3, 8, 128), bf16),
            V((nw, 1, 128), I32), V((nw, 1, 128), I32),
            V((nw, 16, 128), I32), V((nw, 16, 128), I32),
            V((nw, 32, 128), I32), V((nw, 32, 128), I32),
            V((nw, SAMPLES, 16, 128), I32), V((nw, SAMPLES, 16, 128), I32),
            V((3, LROWS, 128), F32), V((4 * S, 128), F32),
            D((6,)), D((ng,)), D((ng,)), D((ng,)), D((ng,)), D((nw,)), D((nw,)), D((nw,)), D((nw,)), D((nw,)), D((nw,)),
        ],
        compiler_params=pltpu.CompilerParams(
            collective_id=0, has_side_effects=True, vmem_limit_bytes=67043328
        ),
    )(
        surf_depth[0, 0],
        jnp.transpose(surf_color[0, 0], (1, 0, 2)),
        surf_box[0, 0].T,
        jnp.transpose(vol_color[0, 0], (0, 2, 1, 3)),
        vol_alpha[0, 0],
        vol_box[0, 0].T,
        ray_entry[0, 0],
        ray_step[0, 0],
        order,
    )
    return frame[None, None]


def solution(mesh):
    nw, ng = mesh.shape["wide"], mesh.shape["grp"]
    nx = max(d for d in range(1, nw + 1) if d * d <= nw and nw % d == 0)
    dims = (nx, nw // nx, ng // 2, 2)
    return jax.shard_map(
        functools.partial(per_device, dims),
        mesh=mesh,
        in_specs=(
            P("wide", "grp", None, None),
            P("wide", "grp", None, None, None),
            P("wide", "grp", None, None),
            P("wide", "grp", None, None, None, None),
            P("wide", "grp", None, None, None),
            P("wide", "grp", None, None),
            P("wide", "grp", None, None),
            P("wide", "grp", None, None),
            P("grp", None),
        ),
        out_specs=P("grp", "wide", None, None),
        check_vma=False,
    )
```

```python
import functools

import jax
import jax.numpy as jnp
from jax import lax
from jax.experimental import pallas as pl
from jax.experimental.pallas import tpu as pltpu
from jax.sharding import PartitionSpec as P

MESH = pl.DeviceIdType.MESH
FAR = 1073741824
PIX = 4096
LROWS = 32
S = 40
SAMPLES = 8
COLOR_SCALE = 59000.0
ALPHA_SCALE = 236000.0

I32 = jnp.int32
F32 = jnp.float32


def far_first(nx, ny):
    ring = lambda d, n: min(d, n - d)
    offsets = [(a, b) for a in range(nx) for b in range(ny) if (a, b) != (0, 0)]
    return sorted(offsets, key=lambda o: -(ring(o[0], nx) + ring(o[1], ny)))


def kernel(
    dims,
    sdepth, scolor, sbox_hbm, vcolor, valpha, vbox_hbm, entry, step, order_hbm,
    out,
    sbox, vbox, order,
    sd_nat, sc_nat, vc_nat, va_nat, en_nat, st_nat,
    sd, sc, en, st, ad, cd,
    a_send, a_recv, c_send, c_recv, t_send, t_recv, l_send, l_recv, f_send, f_recv,
    tab0, tab1, surf, od,
    lsem, g_ready, w_ready, a_ss, a_rs, c_ss, c_rs, t_ss, t_rs, l_ss, l_rs, f_ss, f_rs,
):
    nx, ny, nz, ncore = dims
    nw, ng = nx * ny, nz * ncore
    me_w, me_g = lax.axis_index("wide"), lax.axis_index("grp")
    wide_offsets, grp_offsets = far_first(nx, ny), far_first(nz, ncore)

    def wide_peer(o):
        x, y = me_w // ny, me_w % ny
        return ((x + o[0]) % nx) * ny + (y + o[1]) % ny

    def grp_peer(o):
        z, core = me_g // ncore, me_g % ncore
        return ((z + o[0]) % nz) * ncore + (core + o[1]) % ncore

    def wide_copy(peer, src, dst, ss, rs):
        return pltpu.make_async_remote_copy(
            src_ref=src.at[peer], dst_ref=dst.at[me_w], send_sem=ss, recv_sem=rs,
            device_id=(peer, me_g), device_id_type=MESH,
        )

    def grp_copy(peer, src, dst, ss, rs):
        return pltpu.make_async_remote_copy(
            src_ref=src.at[peer], dst_ref=dst.at[me_g], send_sem=ss, recv_sem=rs,
            device_id=(me_w, peer), device_id_type=MESH,
        )

    def all_of(n, buf, sem):
        pltpu.make_async_copy(buf.at[pl.ds(0, n)], buf.at[pl.ds(0, n)], sem).wait()

    half = ng // 2
    barrier = pltpu.get_barrier_semaphore()

    def greet(sem_g, sem_w, wants):
        for o in grp_offsets:
            peer = grp_peer(o)

            @pl.when(wants(peer, me_g))
            def _():
                pl.semaphore_signal(sem_g, inc=1, device_id=(me_w, peer), device_id_type=MESH)

        for o in wide_offsets:
            peer = wide_peer(o)

            @pl.when(wants(peer, me_w))
            def _():
                pl.semaphore_signal(sem_w, inc=1, device_id=(peer, me_g), device_id_type=MESH)

    loads = []
    for i, (src, dst) in enumerate(
        (
            (sbox_hbm, sbox), (sdepth, sd_nat), (vbox_hbm, vbox), (order_hbm, order), (scolor, sc_nat),
            (valpha, va_nat), (vcolor, vc_nat), (entry, en_nat), (step, st_nat),
        )
    ):
        loads.append(pltpu.make_async_copy(src, dst, lsem.at[i]))
        if i < 4:
            loads[-1].start()
    greet(barrier, barrier, lambda peer, me: peer > me)
    for load in loads[4:]:
        load.start()

    def send_where(offsets, peer_of, me, copy, wants, *bufs):
        for o in offsets:
            pl.when(wants(peer_of(o), me))(lambda o=o: copy(peer_of(o), *bufs).start())

    lower, higher = (lambda peer, me: peer < me), (lambda peer, me: peer > me)

    row8 = lax.broadcasted_iota(I32, (8, 128), 0)
    lane8 = lax.broadcasted_iota(I32, (8, 128), 1)
    fold8 = 2 * row8 + (lane8 >> 6)
    col8 = lane8 & 63
    fold16 = 2 * lax.broadcasted_iota(I32, (16, 128), 0) + (lax.broadcasted_iota(I32, (16, 128), 1) >> 6)
    col16 = lax.broadcasted_iota(I32, (16, 128), 1) & 63

    def spread(nat, dense, n, lead=()):
        g = min(8, n)
        for h in range(n // g):
            for j in range(LROWS):
                tile = nat[(*lead, pl.ds(h * g, g), pl.ds(128 * j, 128))]
                if tile.dtype == jnp.bfloat16:
                    tile = tile.astype(F32)
                dense[pl.ds(h * g * S + j, g, stride=S), :] = tile

    loads[0].wait()
    loads[1].wait()
    spread(sd_nat, sd, ng)

    def surface_inside(r):
        inx = (col8 >= sbox[2, r]) & (col8 < sbox[3, r])
        return [
            inx & (fold8 + 16 * q >= sbox[0, r]) & (fold8 + 16 * q < sbox[1, r]) for q in range(4)
        ]

    for r in range(ng):
        folded = jnp.full((8, 128), FAR, I32)
        for q, inside in enumerate(surface_inside(r)):
            folded = jnp.where(inside, sd[pl.ds(r * S + 8 * q, 8), :], folded)
        a_send[r, 0:8, :] = folded
        a_send[r, 8:9, :] = jnp.full((1, 128), sbox[0, r], I32)
    loads[2].wait()
    for c in range(nw):
        t_send[c] = jnp.full((1, 128), vbox[0, c], I32)
    a_recv[me_g] = a_send[me_g]
    t_recv[me_w] = t_send[me_w]

    pl.when(me_g + me_w > 0)(lambda: pl.semaphore_wait(barrier, me_g + me_w))
    greet(g_ready, w_ready, lambda peer, me: peer < me)

    send_where(grp_offsets, grp_peer, me_g, grp_copy, lower, a_send, a_recv, a_ss, a_rs.at[me_g // half])
    send_where(wide_offsets, wide_peer, me_w, wide_copy, lower, t_send, t_recv, t_ss, t_rs)

    loads[4].wait()
    for ch in range(3):
        spread(sc_nat, sc.at[ch], ng, (ch,))

    def fold_color(r, carry):
        inside = surface_inside(r)
        for ch in range(3):
            folded = jnp.zeros((8, 128), F32)
            for q in range(4):
                folded = jnp.where(inside[q], sc[ch, pl.ds(r * S + 8 * q, 8), :], folded)
            c_send[r, ch] = folded.astype(jnp.bfloat16)
        return carry

    lax.fori_loop(0, ng, fold_color, 0)
    c_recv[me_g] = c_send[me_g]

    for load in loads[5:]:
        load.wait()
    spread(en_nat, en, nw)
    spread(st_nat, st, nw)

    lane1 = lax.broadcasted_iota(I32, (8, 128), 1) >> 6

    def prefixes(c, carry):
        top, bottom = vbox[0, c], vbox[1, c]
        for j in range(16):
            s = lane1 + 2 * j
            upper = (top + ((s - top) & 31)) >= 32
            px, px2 = pl.ds(128 * j, 128), pl.ds(128 * (j + 16), 128)
            ad[pl.ds(j, SAMPLES, stride=S), :] = jnp.where(
                upper, va_nat[c, :, px2].astype(F32), va_nat[c, :, px].astype(F32)
            )
            for ch in range(3):
                cd[ch, pl.ds(j, SAMPLES, stride=S), :] = jnp.where(
                    upper, vc_nat[c, ch, :, px2].astype(F32), vc_nat[c, ch, :, px].astype(F32)
                )
        y = top + ((fold16 - top) & 31)
        upper = y >= 32
        inside = (y < bottom) & (col16 >= vbox[2, c]) & (col16 < vbox[3, c])
        first = jnp.where(upper, en[pl.ds(c * S + 16, 16), :], en[pl.ds(c * S, 16), :])
        en[pl.ds(c * S, 16), :] = jnp.where(inside, first, FAR)
        st[pl.ds(c * S, 16), :] = jnp.where(upper, st[pl.ds(c * S + 16, 16), :], st[pl.ds(c * S, 16), :])
        trans = jnp.ones((16, 128), F32)
        accum = [jnp.zeros((16, 128), F32) for _ in range(3)]
        for k in range(SAMPLES):
            alpha = ad[pl.ds(k * S, 16), :]
            weight = trans * alpha
            trans = trans * (1.0 - alpha)
            for ch in range(3):
                accum[ch] = accum[ch] + weight * cd[ch, pl.ds(k * S, 16), :]
            r, g, b = [(a * COLOR_SCALE + 0.5).astype(I32) for a in accum]
            t = ((1.0 - trans) * ALPHA_SCALE + 0.5).astype(I32)
            tab0[c, k] = (r << 16) | g
            tab1[c, k] = (b << 16) | t
        return carry

    lax.fori_loop(0, nw, prefixes, 0)

    pl.when(me_w < nw - 1)(lambda: pl.semaphore_wait(w_ready, nw - 1 - me_w))
    send_where(wide_offsets, wide_peer, me_w, wide_copy, higher, t_send, t_recv, t_ss, t_rs)
    pl.when(me_g < ng - 1)(lambda: pl.semaphore_wait(g_ready, ng - 1 - me_g))
    send_where(grp_offsets, grp_peer, me_g, grp_copy, higher, a_send, a_recv, a_ss, a_rs.at[me_g // half])

    near = [jnp.full((8, 128), FAR, I32) for _ in range(4)]
    winner = [jnp.full((8, 128), -1, I32) for _ in range(4)]
    for s in range(ng):
        if s % half == 0:
            own = me_g // half == s // half
            pl.when(own)(lambda: all_of(half - 1, a_recv, a_rs.at[s // half]))
            pl.when(jnp.logical_not(own))(lambda: all_of(half, a_recv, a_rs.at[s // half]))
        depth = a_recv[s, 0:8, :]
        top = a_recv[s, 8:9, :]
        where_q = (top + ((fold8 - top) & 15)) >> 4
        for q in range(4):
            take = (where_q == q) & (depth < near[q])
            near[q] = jnp.where(take, depth, near[q])
            winner[q] = jnp.where(take, s, winner[q])

    all_of(nw - 1, t_recv, t_rs)

    def upper_half(top):
        return (top + ((fold16 - top) & 31)) >= 32

    near_lo = jnp.concatenate(near[:2], axis=0)
    near_hi = jnp.concatenate(near[2:], axis=0)
    for b in range(nw):
        l_send[b] = jnp.where(upper_half(t_recv[b]), near_hi, near_lo)
    l_recv[me_w] = l_send[me_w]
    for o in wide_offsets:
        wide_copy(wide_peer(o), l_send, l_recv, l_ss, l_rs.at[me_w]).start()
    for o in grp_offsets:
        grp_copy(grp_peer(o), c_send, c_recv, c_ss, c_rs).start()

    def by_start():
        for k in range(nx + ny - 1):
            low, high = max(0, k - ny + 1), min(nx - 1, k)
            for i in range(high - low + 1):
                x = low + (me_w // ny + me_w % ny + i) % (high - low + 1)
                yield x * ny + k - x

    for c in by_start():
        pl.when(me_w != c)(lambda c=c: pltpu.make_async_copy(l_recv.at[c], l_recv.at[c], l_rs.at[c]).wait())
        limit = l_recv[c]
        at = en[pl.ds(c * S, 16), :]
        stride = st[pl.ds(c * S, 16), :]
        word0 = jnp.zeros((16, 128), I32)
        word1 = jnp.zeros((16, 128), I32)
        for k in range(SAMPLES):
            kept = at < limit
            word0 = jnp.where(kept, tab0[c, k], word0)
            word1 = jnp.where(kept, tab1[c, k], word1)
            at = at + stride
        f_send[c, 0:16, :] = word0
        f_send[c, 16:32, :] = word1

        @pl.when(me_w != c)
        def _(c=c):
            wide_copy(c, f_send, f_recv, f_ss, f_rs).start()

    f_recv[me_w] = f_send[me_w]
    all_of(ng - 1, c_recv, c_rs)
    color = [[jnp.zeros((8, 128), F32) for _ in range(3)] for _ in range(4)]
    for s in range(ng):
        rgb = [c_recv[s, ch].astype(F32) for ch in range(3)]
        for q in range(4):
            won = winner[q] == s
            color[q] = [jnp.where(won, rgb[ch], color[q][ch]) for ch in range(3)]
    for ch in range(3):
        for q in range(4):
            surf[ch, 8 * q : 8 * q + 8, :] = color[q][ch]

    all_of(nw - 1, f_recv, f_rs)
    through = [jnp.ones((16, 128), F32) for _ in range(2)]
    total = [[jnp.zeros((16, 128), F32) for _ in range(3)] for _ in range(2)]
    loads[3].wait()
    for j in range(nw):
        b = order[0, j]
        word0, word1 = f_recv[b, 0:16, :], f_recv[b, 16:32, :]
        upper = upper_half(t_recv[b])
        layer = [
            lax.shift_right_logical(word0, 16).astype(F32),
            (word0 & 65535).astype(F32),
            lax.shift_right_logical(word1, 16).astype(F32),
        ]
        opaque = (word1 & 65535).astype(F32) * (1.0 / ALPHA_SCALE)
        for h in range(2):
            weight = jnp.where(upper, through[h], 0.0) if h else jnp.where(upper, 0.0, through[h])
            total[h] = [total[h][ch] + weight * layer[ch] for ch in range(3)]
            through[h] = through[h] - weight * opaque
    for h in range(2):
        rows = slice(16 * h, 16 * h + 16)
        for ch in range(3):
            od[ch * S + 16 * h : ch * S + 16 * h + 16, :] = (
                total[h][ch] * (1.0 / COLOR_SCALE) + through[h] * surf[ch, rows, :]
            )
        od[3 * S + 16 * h : 3 * S + 16 * h + 16, :] = through[h]
    for j in range(LROWS):
        out[:, 128 * j : 128 * j + 128] = od[pl.ds(j, 4, stride=S), :]

    for n, buf, sem in (
        (ng - 1, a_send, a_ss), (ng - 1, c_send, c_ss), (nw - 1, t_send, t_ss), (nw - 1, l_send, l_ss), (nw - 1, f_send, f_ss),
    ):
        all_of(n, buf, sem)


def per_device(dims, surf_depth, surf_color, surf_box, vol_color, vol_alpha, vol_box, ray_entry, ray_step, order):
    nx, ny, nz, ncore = dims
    nw, ng = nx * ny, nz * ncore
    V, D = pltpu.VMEM, pltpu.SemaphoreType.DMA
    bf16 = jnp.bfloat16
    hbm = pl.BlockSpec(memory_space=pltpu.HBM)
    frame = pl.pallas_call(
        functools.partial(kernel, dims),
        out_shape=pltpu.VMEM((4, PIX), F32),
        in_specs=[hbm] * 9,
        out_specs=pl.BlockSpec(memory_space=pltpu.VMEM),
        scratch_shapes=[
            pltpu.SMEM((4, ng), I32), pltpu.SMEM((4, nw), I32), pltpu.SMEM((1, nw), I32),
            V((ng, PIX), I32), V((3, ng, PIX), bf16), V((nw, 3, SAMPLES, PIX), bf16), V((nw, SAMPLES, PIX), bf16),
            V((nw, PIX), I32), V((nw, PIX), I32),
            V((ng * S, 128), I32), V((3, ng * S, 128), F32), V((nw * S, 128), I32), V((nw * S, 128), I32),
            V((SAMPLES * S, 128), F32), V((3, SAMPLES * S, 128), F32),
            V((ng, 9, 128), I32), V((ng, 9, 128), I32),
            V((ng, 3, 8, 128), bf16), V((ng, 3, 8, 128), bf16),
            V((nw, 1, 128), I32), V((nw, 1, 128), I32),
            V((nw, 16, 128), I32), V((nw, 16, 128), I32),
            V((nw, 32, 128), I32), V((nw, 32, 128), I32),
            V((nw, SAMPLES, 16, 128), I32), V((nw, SAMPLES, 16, 128), I32),
            V((3, LROWS, 128), F32), V((4 * S, 128), F32),
            D((9,)), pltpu.SemaphoreType.REGULAR, pltpu.SemaphoreType.REGULAR,
            D, D((2,)), D, D, D, D, D, D((nw,)), D, D,
        ],
        compiler_params=pltpu.CompilerParams(
            collective_id=0, has_side_effects=True, vmem_limit_bytes=66977792
        ),
    )(
        surf_depth[0, 0],
        jnp.transpose(surf_color[0, 0], (1, 0, 2)),
        surf_box[0, 0].T,
        jnp.transpose(vol_color[0, 0], (0, 2, 1, 3)),
        vol_alpha[0, 0],
        vol_box[0, 0].T,
        ray_entry[0, 0],
        ray_step[0, 0],
        order,
    )
    return frame[None, None]


def solution(mesh):
    nw, ng = mesh.shape["wide"], mesh.shape["grp"]
    nx = max(d for d in range(1, nw + 1) if d * d <= nw and nw % d == 0)
    dims = (nx, nw // nx, ng // 2, 2)
    return jax.shard_map(
        functools.partial(per_device, dims),
        mesh=mesh,
        in_specs=(
            P("wide", "grp", None, None),
            P("wide", "grp", None, None, None),
            P("wide", "grp", None, None),
            P("wide", "grp", None, None, None, None),
            P("wide", "grp", None, None, None),
            P("wide", "grp", None, None),
            P("wide", "grp", None, None),
            P("wide", "grp", None, None),
            P("grp", None),
        ),
        out_specs=P("grp", "wide", None, None),
        check_vma=False,
    )
```

```python
import functools

import jax
import jax.numpy as jnp
from jax import lax
from jax.experimental import pallas as pl
from jax.experimental.pallas import tpu as pltpu
from jax.sharding import PartitionSpec as P

MESH = pl.DeviceIdType.MESH
FAR = 1073741824
PIX = 4096
LROWS = 32
S = 40
SAMPLES = 8
COLOR_SCALE = 59000.0
ALPHA_SCALE = 236000.0

I32 = jnp.int32
F32 = jnp.float32


def far_first(nx, ny):
    ring = lambda d, n: min(d, n - d)
    offsets = [(a, b) for a in range(nx) for b in range(ny) if (a, b) != (0, 0)]
    return sorted(offsets, key=lambda o: -(ring(o[0], nx) + ring(o[1], ny)))


def kernel(
    dims,
    sdepth, scolor, sbox_hbm, vcolor, valpha, vbox_hbm, entry, step, order_hbm,
    out,
    sbox, vbox, order,
    sd_nat, sc_nat, vc_nat, va_nat, en_nat, st_nat,
    sd, sc, en, st, ad, cd,
    a_send, a_recv, c_send, c_recv, l_send, l_recv, f_send, f_recv,
    tab0, tab1, surf, od,
    lsem, g_ready, w_ready, a_ss, a_rs, c_ss, c_rs, l_ss, l_rs, f_ss, f_rs,
):
    nx, ny, nz, ncore = dims
    nw, ng = nx * ny, nz * ncore
    me_w, me_g = lax.axis_index("wide"), lax.axis_index("grp")
    wide_offsets, grp_offsets = far_first(nx, ny), far_first(nz, ncore)

    def wide_peer(o):
        x, y = me_w // ny, me_w % ny
        return ((x + o[0]) % nx) * ny + (y + o[1]) % ny

    def grp_peer(o):
        z, core = me_g // ncore, me_g % ncore
        return ((z + o[0]) % nz) * ncore + (core + o[1]) % ncore

    def wide_copy(peer, src, dst, ss, rs):
        return pltpu.make_async_remote_copy(
            src_ref=src.at[peer], dst_ref=dst.at[me_w], send_sem=ss, recv_sem=rs,
            device_id=(peer, me_g), device_id_type=MESH,
        )

    def grp_copy(peer, src, dst, ss, rs):
        return pltpu.make_async_remote_copy(
            src_ref=src.at[peer], dst_ref=dst.at[me_g], send_sem=ss, recv_sem=rs,
            device_id=(me_w, peer), device_id_type=MESH,
        )

    def all_of(n, buf, sem):
        pltpu.make_async_copy(buf.at[pl.ds(0, n)], buf.at[pl.ds(0, n)], sem).wait()

    half = ng // 2
    barrier = pltpu.get_barrier_semaphore()

    def tell(sem, w, g):
        pl.semaphore_signal(sem, inc=1, device_id=(w, g), device_id_type=MESH)

    def tell_grp(sem, wants):
        for o in grp_offsets:
            peer = grp_peer(o)
            pl.when(wants(peer))(lambda peer=peer: tell(sem, me_w, peer))

    def tell_plane(sem):
        @pl.when(me_w == 0)
        def _():
            for o in wide_offsets:
                tell(sem, wide_peer(o), me_g)

    loads = []
    for i, (src, dst) in enumerate(
        (
            (sbox_hbm, sbox), (sdepth, sd_nat), (vbox_hbm, vbox), (order_hbm, order), (scolor, sc_nat),
            (valpha, va_nat), (vcolor, vc_nat), (entry, en_nat), (step, st_nat),
        )
    ):
        loads.append(pltpu.make_async_copy(src, dst, lsem.at[i]))
        if i < 4:
            loads[-1].start()
    tell_grp(barrier, lambda peer: peer > me_g)
    tell_plane(barrier)
    for load in loads[4:]:
        load.start()

    def send_where(offsets, peer_of, me, copy, wants, *bufs):
        for o in offsets:
            pl.when(wants(peer_of(o), me))(lambda o=o: copy(peer_of(o), *bufs).start())

    lower, higher = (lambda peer, me: peer < me), (lambda peer, me: peer > me)

    row8 = lax.broadcasted_iota(I32, (8, 128), 0)
    lane8 = lax.broadcasted_iota(I32, (8, 128), 1)
    fold8 = 2 * row8 + (lane8 >> 6)
    col8 = lane8 & 63
    fold16 = 2 * lax.broadcasted_iota(I32, (16, 128), 0) + (lax.broadcasted_iota(I32, (16, 128), 1) >> 6)
    col16 = lax.broadcasted_iota(I32, (16, 128), 1) & 63

    def spread(nat, dense, n, lead=()):
        g = min(8, n)
        for h in range(n // g):
            for j in range(LROWS):
                tile = nat[(*lead, pl.ds(h * g, g), pl.ds(128 * j, 128))]
                if tile.dtype == jnp.bfloat16:
                    tile = tile.astype(F32)
                dense[pl.ds(h * g * S + j, g, stride=S), :] = tile

    loads[0].wait()
    loads[1].wait()
    spread(sd_nat, sd, ng)

    def surface_inside(r):
        inx = (col8 >= sbox[2, r]) & (col8 < sbox[3, r])
        return [
            inx & (fold8 + 16 * q >= sbox[0, r]) & (fold8 + 16 * q < sbox[1, r]) for q in range(4)
        ]

    for r in range(ng):
        folded = jnp.full((8, 128), FAR, I32)
        for q, inside in enumerate(surface_inside(r)):
            folded = jnp.where(inside, sd[pl.ds(r * S + 8 * q, 8), :], folded)
        a_send[r, 0:8, :] = folded
        a_send[r, 8:9, :] = jnp.full((1, 128), sbox[0, r], I32)
    a_recv[me_g] = a_send[me_g]

    entered = me_g + (me_w > 0).astype(I32)
    pl.when(entered > 0)(lambda: pl.semaphore_wait(barrier, entered))
    tell_grp(g_ready, lambda peer: peer < me_g)
    pl.when(me_w > 0)(lambda: tell(w_ready, 0, me_g))

    def send_depths(wants):
        for o in grp_offsets:
            peer = grp_peer(o)
            pl.when(wants(peer))(lambda peer=peer: grp_copy(peer, a_send, a_recv, a_ss, a_rs.at[me_g // half]).start())

    send_depths(lambda peer: peer < me_g)

    loads[4].wait()
    for ch in range(3):
        spread(sc_nat, sc.at[ch], ng, (ch,))

    def fold_color(r, carry):
        inside = surface_inside(r)
        for ch in range(3):
            folded = jnp.zeros((8, 128), F32)
            for q in range(4):
                folded = jnp.where(inside[q], sc[ch, pl.ds(r * S + 8 * q, 8), :], folded)
            c_send[r, ch] = folded.astype(jnp.bfloat16)
        return carry

    lax.fori_loop(0, ng, fold_color, 0)
    c_recv[me_g] = c_send[me_g]

    for load in (loads[2], *loads[5:]):
        load.wait()
    spread(en_nat, en, nw)
    spread(st_nat, st, nw)

    lane1 = lax.broadcasted_iota(I32, (8, 128), 1) >> 6

    def prefixes(c, carry):
        top, bottom = vbox[0, c], vbox[1, c]
        for j in range(16):
            s = lane1 + 2 * j
            upper = (top + ((s - top) & 31)) >= 32
            px, px2 = pl.ds(128 * j, 128), pl.ds(128 * (j + 16), 128)
            ad[pl.ds(j, SAMPLES, stride=S), :] = jnp.where(
                upper, va_nat[c, :, px2].astype(F32), va_nat[c, :, px].astype(F32)
            )
            for ch in range(3):
                cd[ch, pl.ds(j, SAMPLES, stride=S), :] = jnp.where(
                    upper, vc_nat[c, ch, :, px2].astype(F32), vc_nat[c, ch, :, px].astype(F32)
                )
        y = top + ((fold16 - top) & 31)
        upper = y >= 32
        inside = (y < bottom) & (col16 >= vbox[2, c]) & (col16 < vbox[3, c])
        first = jnp.where(upper, en[pl.ds(c * S + 16, 16), :], en[pl.ds(c * S, 16), :])
        en[pl.ds(c * S, 16), :] = jnp.where(inside, first, FAR)
        st[pl.ds(c * S, 16), :] = jnp.where(upper, st[pl.ds(c * S + 16, 16), :], st[pl.ds(c * S, 16), :])
        trans = jnp.ones((16, 128), F32)
        accum = [jnp.zeros((16, 128), F32) for _ in range(3)]
        for k in range(SAMPLES):
            alpha = ad[pl.ds(k * S, 16), :]
            weight = trans * alpha
            trans = trans * (1.0 - alpha)
            for ch in range(3):
                accum[ch] = accum[ch] + weight * cd[ch, pl.ds(k * S, 16), :]
            r, g, b = [(a * COLOR_SCALE + 0.5).astype(I32) for a in accum]
            t = ((1.0 - trans) * ALPHA_SCALE + 0.5).astype(I32)
            tab0[c, k] = (r << 16) | g
            tab1[c, k] = (b << 16) | t
        return carry

    lax.fori_loop(0, nw, prefixes, 0)

    @pl.when(me_w == 0)
    def _():
        pl.semaphore_wait(w_ready, nw - 1)

    tell_plane(w_ready)
    pl.when(me_g < ng - 1)(lambda: pl.semaphore_wait(g_ready, ng - 1 - me_g))
    send_depths(lambda peer: peer > me_g)

    near = [jnp.full((8, 128), FAR, I32) for _ in range(4)]
    winner = [jnp.full((8, 128), -1, I32) for _ in range(4)]
    for s in range(ng):
        if s % half == 0:
            own = me_g // half == s // half
            pl.when(own)(lambda: all_of(half - 1, a_recv, a_rs.at[s // half]))
            pl.when(jnp.logical_not(own))(lambda: all_of(half, a_recv, a_rs.at[s // half]))
        depth = a_recv[s, 0:8, :]
        top = a_recv[s, 8:9, :]
        where_q = (top + ((fold8 - top) & 15)) >> 4
        for q in range(4):
            take = (where_q == q) & (depth < near[q])
            near[q] = jnp.where(take, depth, near[q])
            winner[q] = jnp.where(take, s, winner[q])

    def upper_half(top):
        return (top + ((fold16 - top) & 31)) >= 32

    for q in range(4):
        l_send[8 * q : 8 * q + 8, :] = near[q]
    l_recv[me_w] = l_send[...]
    pl.when(me_w > 0)(lambda: pl.semaphore_wait(w_ready, 1))
    for o in wide_offsets:
        pltpu.make_async_remote_copy(
            src_ref=l_send, dst_ref=l_recv.at[me_w], send_sem=l_ss, recv_sem=l_rs.at[me_w],
            device_id=(wide_peer(o), me_g), device_id_type=MESH,
        ).start()
    for o in grp_offsets:
        grp_copy(grp_peer(o), c_send, c_recv, c_ss, c_rs).start()

    def by_start():
        for k in range(nx + ny - 1):
            low, high = max(0, k - ny + 1), min(nx - 1, k)
            for i in range(high - low + 1):
                x = low + (me_w // ny + me_w % ny + i) % (high - low + 1)
                yield x * ny + k - x

    for c in by_start():
        pl.when(me_w != c)(lambda c=c: pltpu.make_async_copy(l_recv.at[c], l_recv.at[c], l_rs.at[c]).wait())
        limit = jnp.where(upper_half(vbox[0, c]), l_recv[c, 16:32, :], l_recv[c, 0:16, :])
        at = en[pl.ds(c * S, 16), :]
        stride = st[pl.ds(c * S, 16), :]
        word0 = jnp.zeros((16, 128), I32)
        word1 = jnp.zeros((16, 128), I32)
        for k in range(SAMPLES):
            kept = at < limit
            word0 = jnp.where(kept, tab0[c, k], word0)
            word1 = jnp.where(kept, tab1[c, k], word1)
            at = at + stride
        f_send[c, 0:16, :] = word0
        f_send[c, 16:32, :] = word1
        f_send[c, 32:33, :] = jnp.full((1, 128), vbox[0, c], I32)

        @pl.when(me_w != c)
        def _(c=c):
            wide_copy(c, f_send, f_recv, f_ss, f_rs).start()

    f_recv[me_w] = f_send[me_w]
    all_of(ng - 1, c_recv, c_rs)
    color = [[jnp.zeros((8, 128), F32) for _ in range(3)] for _ in range(4)]
    for s in range(ng):
        rgb = [c_recv[s, ch].astype(F32) for ch in range(3)]
        for q in range(4):
            won = winner[q] == s
            color[q] = [jnp.where(won, rgb[ch], color[q][ch]) for ch in range(3)]
    for ch in range(3):
        for q in range(4):
            surf[ch, 8 * q : 8 * q + 8, :] = color[q][ch]

    all_of(nw - 1, f_recv, f_rs)
    through = [jnp.ones((16, 128), F32) for _ in range(2)]
    total = [[jnp.zeros((16, 128), F32) for _ in range(3)] for _ in range(2)]
    loads[3].wait()
    for j in range(nw):
        b = order[0, j]
        word0, word1 = f_recv[b, 0:16, :], f_recv[b, 16:32, :]
        upper = upper_half(f_recv[b, 32:33, :])
        layer = [
            lax.shift_right_logical(word0, 16).astype(F32),
            (word0 & 65535).astype(F32),
            lax.shift_right_logical(word1, 16).astype(F32),
        ]
        opaque = (word1 & 65535).astype(F32) * (1.0 / ALPHA_SCALE)
        for h in range(2):
            weight = jnp.where(upper, through[h], 0.0) if h else jnp.where(upper, 0.0, through[h])
            total[h] = [total[h][ch] + weight * layer[ch] for ch in range(3)]
            through[h] = through[h] - weight * opaque
    for h in range(2):
        rows = slice(16 * h, 16 * h + 16)
        for ch in range(3):
            od[ch * S + 16 * h : ch * S + 16 * h + 16, :] = (
                total[h][ch] * (1.0 / COLOR_SCALE) + through[h] * surf[ch, rows, :]
            )
        od[3 * S + 16 * h : 3 * S + 16 * h + 16, :] = through[h]
    for j in range(LROWS):
        out[:, 128 * j : 128 * j + 128] = od[pl.ds(j, 4, stride=S), :]

    for n, buf, sem in (
        (ng - 1, a_send, a_ss), (ng - 1, c_send, c_ss), (nw - 1, l_recv, l_ss), (nw - 1, f_send, f_ss),
    ):
        all_of(n, buf, sem)


def per_device(dims, surf_depth, surf_color, surf_box, vol_color, vol_alpha, vol_box, ray_entry, ray_step, order):
    nx, ny, nz, ncore = dims
    nw, ng = nx * ny, nz * ncore
    V, D = pltpu.VMEM, pltpu.SemaphoreType.DMA
    bf16 = jnp.bfloat16
    hbm = pl.BlockSpec(memory_space=pltpu.HBM)
    frame = pl.pallas_call(
        functools.partial(kernel, dims),
        out_shape=pltpu.VMEM((4, PIX), F32),
        in_specs=[hbm] * 9,
        out_specs=pl.BlockSpec(memory_space=pltpu.VMEM),
        scratch_shapes=[
            pltpu.SMEM((4, ng), I32), pltpu.SMEM((4, nw), I32), pltpu.SMEM((1, nw), I32),
            V((ng, PIX), I32), V((3, ng, PIX), bf16), V((nw, 3, SAMPLES, PIX), bf16), V((nw, SAMPLES, PIX), bf16),
            V((nw, PIX), I32), V((nw, PIX), I32),
            V((ng * S, 128), I32), V((3, ng * S, 128), F32), V((nw * S, 128), I32), V((nw * S, 128), I32),
            V((SAMPLES * S, 128), F32), V((3, SAMPLES * S, 128), F32),
            V((ng, 9, 128), I32), V((ng, 9, 128), I32),
            V((ng, 3, 8, 128), bf16), V((ng, 3, 8, 128), bf16),
            V((LROWS, 128), I32), V((nw, LROWS, 128), I32),
            V((nw, 33, 128), I32), V((nw, 33, 128), I32),
            V((nw, SAMPLES, 16, 128), I32), V((nw, SAMPLES, 16, 128), I32),
            V((3, LROWS, 128), F32), V((4 * S, 128), F32),
            D((9,)), pltpu.SemaphoreType.REGULAR, pltpu.SemaphoreType.REGULAR,
            D, D((2,)), D, D, D, D((nw,)), D, D,
        ],
        compiler_params=pltpu.CompilerParams(
            collective_id=0, has_side_effects=True, vmem_limit_bytes=66977792
        ),
    )(
        surf_depth[0, 0],
        jnp.transpose(surf_color[0, 0], (1, 0, 2)),
        surf_box[0, 0].T,
        jnp.transpose(vol_color[0, 0], (0, 2, 1, 3)),
        vol_alpha[0, 0],
        vol_box[0, 0].T,
        ray_entry[0, 0],
        ray_step[0, 0],
        order,
    )
    return frame[None, None]


def solution(mesh):
    nw, ng = mesh.shape["wide"], mesh.shape["grp"]
    nx = max(d for d in range(1, nw + 1) if d * d <= nw and nw % d == 0)
    dims = (nx, nw // nx, ng // 2, 2)
    return jax.shard_map(
        functools.partial(per_device, dims),
        mesh=mesh,
        in_specs=(
            P("wide", "grp", None, None),
            P("wide", "grp", None, None, None),
            P("wide", "grp", None, None),
            P("wide", "grp", None, None, None, None),
            P("wide", "grp", None, None, None),
            P("wide", "grp", None, None),
            P("wide", "grp", None, None),
            P("wide", "grp", None, None),
            P("grp", None),
        ),
        out_specs=P("grp", "wide", None, None),
        check_vma=False,
    )
```

```python
import functools

import jax
import jax.numpy as jnp
from jax import lax
from jax.experimental import pallas as pl
from jax.experimental.pallas import tpu as pltpu
from jax.sharding import PartitionSpec as P

MESH = pl.DeviceIdType.MESH
FAR = 1073741824
PIX = 4096
LROWS = 32
S = 40
SAMPLES = 8
COLOR_SCALE = 59000.0
ALPHA_SCALE = 236000.0

I32 = jnp.int32
F32 = jnp.float32


def far_first(nx, ny):
    ring = lambda d, n: min(d, n - d)
    offsets = [(a, b) for a in range(nx) for b in range(ny) if (a, b) != (0, 0)]
    return sorted(offsets, key=lambda o: -(ring(o[0], nx) + ring(o[1], ny)))


def kernel(
    dims,
    sdepth, scolor, sbox_hbm, vcolor, valpha, vbox_hbm, entry, step, order_hbm,
    out,
    sbox, vbox, order,
    sd_nat, sc_nat, vc_nat, va_nat, en_nat, st_nat,
    sd, sc, en, st, ad, cd,
    a_send, a_recv, c_send, c_recv, t_send, t_recv, tops_of, l_full, l_send, l_recv, f_send, f_recv,
    tab0, tab1, surf, od,
    lsem, g_ready, w_ready, a_ss, a_rs, c_ss, c_rs, t_ss, t_rs, l_ss, l_rs, f_ss, f_rs,
):
    nx, ny, nz, ncore = dims
    nw, ng = nx * ny, nz * ncore
    me_w, me_g = lax.axis_index("wide"), lax.axis_index("grp")
    wide_offsets, grp_offsets = far_first(nx, ny), far_first(nz, ncore)

    def wide_peer(o):
        x, y = me_w // ny, me_w % ny
        return ((x + o[0]) % nx) * ny + (y + o[1]) % ny

    def grp_peer(o):
        z, core = me_g // ncore, me_g % ncore
        return ((z + o[0]) % nz) * ncore + (core + o[1]) % ncore

    def wide_copy(peer, src, dst, ss, rs):
        return pltpu.make_async_remote_copy(
            src_ref=src.at[peer], dst_ref=dst.at[me_w], send_sem=ss, recv_sem=rs,
            device_id=(peer, me_g), device_id_type=MESH,
        )

    def grp_copy(peer, src, dst, ss, rs):
        return pltpu.make_async_remote_copy(
            src_ref=src.at[peer], dst_ref=dst.at[me_g], send_sem=ss, recv_sem=rs,
            device_id=(me_w, peer), device_id_type=MESH,
        )

    def all_of(n, buf, sem):
        pltpu.make_async_copy(buf.at[pl.ds(0, n)], buf.at[pl.ds(0, n)], sem).wait()

    half = ng // 2
    hub = jnp.where(me_g == 0, ny, 0)
    late = (me_g >= half) & (me_g % 2 == 0)
    barrier = pltpu.get_barrier_semaphore()

    def tell(sem, w, g):
        pl.semaphore_signal(sem, inc=1, device_id=(w, g), device_id_type=MESH)

    def tell_grp(sem, wants):
        for o in grp_offsets:
            peer = grp_peer(o)
            pl.when(wants(peer))(lambda peer=peer: tell(sem, me_w, peer))

    loads = []
    for i, (src, dst) in enumerate(
        (
            (sbox_hbm, sbox), (sdepth, sd_nat), (vbox_hbm, vbox), (order_hbm, order), (scolor, sc_nat),
            (valpha, va_nat), (vcolor, vc_nat), (entry, en_nat), (step, st_nat),
        )
    ):
        loads.append(pltpu.make_async_copy(src, dst, lsem.at[i]))
        if i < 4:
            loads[-1].start()
    tell_grp(barrier, lambda peer: peer > me_g)

    @pl.when(me_w == hub)
    def _():
        for o in wide_offsets:
            tell(barrier, wide_peer(o), me_g)

    for load in loads[4:]:
        load.start()

    def send_where(offsets, peer_of, me, copy, wants, *bufs):
        for o in offsets:
            pl.when(wants(peer_of(o), me))(lambda o=o: copy(peer_of(o), *bufs).start())

    lower, higher = (lambda peer, me: peer < me), (lambda peer, me: peer > me)

    row8 = lax.broadcasted_iota(I32, (8, 128), 0)
    lane8 = lax.broadcasted_iota(I32, (8, 128), 1)
    fold8 = 2 * row8 + (lane8 >> 6)
    col8 = lane8 & 63
    fold16 = 2 * lax.broadcasted_iota(I32, (16, 128), 0) + (lax.broadcasted_iota(I32, (16, 128), 1) >> 6)
    col16 = lax.broadcasted_iota(I32, (16, 128), 1) & 63

    def spread(nat, dense, n, lead=()):
        g = min(8, n)
        for h in range(n // g):
            for j in range(LROWS):
                tile = nat[(*lead, pl.ds(h * g, g), pl.ds(128 * j, 128))]
                if tile.dtype == jnp.bfloat16:
                    tile = tile.astype(F32)
                dense[pl.ds(h * g * S + j, g, stride=S), :] = tile

    loads[2].wait()
    tops = jnp.zeros((1, 128), I32)
    for c in range(nw):
        tops = jnp.where(lax.broadcasted_iota(I32, (1, 128), 1) == c, vbox[0, c], tops)
    t_send[...] = tops
    entered = me_g + (me_w != hub).astype(I32)
    pl.when(entered > 0)(lambda: pl.semaphore_wait(barrier, entered))
    tell_grp(g_ready, lambda peer: peer < me_g)

    @pl.when(me_w != hub)
    def _():
        pltpu.make_async_remote_copy(
            src_ref=t_send, dst_ref=t_recv.at[me_w], send_sem=t_ss, recv_sem=t_rs,
            device_id=(hub, me_g), device_id_type=MESH,
        ).start()

    pl.when(late & (me_w != hub))(lambda: tell(w_ready, hub, me_g))

    loads[0].wait()
    loads[1].wait()
    spread(sd_nat, sd, ng)

    def surface_inside(r):
        inx = (col8 >= sbox[2, r]) & (col8 < sbox[3, r])
        return [
            inx & (fold8 + 16 * q >= sbox[0, r]) & (fold8 + 16 * q < sbox[1, r]) for q in range(4)
        ]

    def send_depth(peer, wanted):
        pl.when(wanted)(lambda: grp_copy(peer, a_send, a_recv, a_ss, a_rs.at[me_g // half]).start())

    def send_color(peer, wanted):
        pl.when(wanted)(lambda: grp_copy(peer, c_send, c_recv, c_ss, c_rs).start())

    for r in range(ng):
        folded = jnp.full((8, 128), FAR, I32)
        for q, inside in enumerate(surface_inside(r)):
            folded = jnp.where(inside, sd[pl.ds(r * S + 8 * q, 8), :], folded)
        a_send[r, 0:8, :] = folded
        a_send[r, 8:9, :] = jnp.full((1, 128), sbox[0, r], I32)
        if r:
            send_depth(r - 1, r - 1 < me_g)
    a_recv[me_g] = a_send[me_g]

    loads[4].wait()
    for ch in range(3):
        spread(sc_nat, sc.at[ch], ng, (ch,))

    def fold_color(r, carry):
        inside = surface_inside(r)
        for ch in range(3):
            folded = jnp.zeros((8, 128), F32)
            for q in range(4):
                folded = jnp.where(inside[q], sc[ch, pl.ds(r * S + 8 * q, 8), :], folded)
            c_send[r, ch] = folded.astype(jnp.bfloat16)
        return carry

    lax.fori_loop(0, ng, fold_color, 0)
    c_recv[me_g] = c_send[me_g]

    for load in loads[5:]:
        load.wait()
    spread(en_nat, en, nw)
    spread(st_nat, st, nw)

    lane1 = lax.broadcasted_iota(I32, (8, 128), 1) >> 6

    def prefixes(c, carry):
        top, bottom = vbox[0, c], vbox[1, c]
        for j in range(16):
            s = lane1 + 2 * j
            upper = (top + ((s - top) & 31)) >= 32
            px, px2 = pl.ds(128 * j, 128), pl.ds(128 * (j + 16), 128)
            ad[pl.ds(j, SAMPLES, stride=S), :] = jnp.where(
                upper, va_nat[c, :, px2].astype(F32), va_nat[c, :, px].astype(F32)
            )
            for ch in range(3):
                cd[ch, pl.ds(j, SAMPLES, stride=S), :] = jnp.where(
                    upper, vc_nat[c, ch, :, px2].astype(F32), vc_nat[c, ch, :, px].astype(F32)
                )
        y = top + ((fold16 - top) & 31)
        upper = y >= 32
        inside = (y < bottom) & (col16 >= vbox[2, c]) & (col16 < vbox[3, c])
        first = jnp.where(upper, en[pl.ds(c * S + 16, 16), :], en[pl.ds(c * S, 16), :])
        en[pl.ds(c * S, 16), :] = jnp.where(inside, first, FAR)
        st[pl.ds(c * S, 16), :] = jnp.where(upper, st[pl.ds(c * S + 16, 16), :], st[pl.ds(c * S, 16), :])
        trans = jnp.ones((16, 128), F32)
        accum = [jnp.zeros((16, 128), F32) for _ in range(3)]
        for k in range(SAMPLES):
            alpha = ad[pl.ds(k * S, 16), :]
            weight = trans * alpha
            trans = trans * (1.0 - alpha)
            for ch in range(3):
                accum[ch] = accum[ch] + weight * cd[ch, pl.ds(k * S, 16), :]
            r, g, b = [(a * COLOR_SCALE + 0.5).astype(I32) for a in accum]
            t = ((1.0 - trans) * ALPHA_SCALE + 0.5).astype(I32)
            tab0[c, k] = (r << 16) | g
            tab1[c, k] = (b << 16) | t
        return carry

    lax.fori_loop(0, nw, prefixes, 0)

    def pass_tops():
        all_of(nw - 1, t_recv, t_rs)
        t_recv[hub] = t_send[...]
        for o in wide_offsets:
            pltpu.make_async_remote_copy(
                src_ref=t_recv, dst_ref=t_recv, send_sem=t_ss, recv_sem=t_rs,
                device_id=(wide_peer(o), me_g), device_id_type=MESH,
            ).start()

    pl.when((me_w == hub) & (me_g < ncore))(pass_tops)
    for o in grp_offsets:
        send_color(grp_peer(o), grp_peer(o) < me_g)
    pl.when(me_g < ng - 1)(lambda: pl.semaphore_wait(g_ready, ng - 1 - me_g))
    for o in grp_offsets:
        send_depth(grp_peer(o), grp_peer(o) > me_g)

    pl.when((me_w == hub) & (me_g >= ncore) & jnp.logical_not(late))(pass_tops)

    @pl.when((me_w == hub) & late)
    def _():
        pl.semaphore_wait(w_ready, nw - 1)
        for o in wide_offsets:
            tell(w_ready, wide_peer(o), me_g)

    near = [jnp.full((8, 128), FAR, I32) for _ in range(4)]
    winner = [jnp.full((8, 128), -1, I32) for _ in range(4)]
    for s in range(ng):
        if s % half == 0:
            own = me_g // half == s // half
            pl.when(own)(lambda: all_of(half - 1, a_recv, a_rs.at[s // half]))
            pl.when(jnp.logical_not(own))(lambda: all_of(half, a_recv, a_rs.at[s // half]))
        depth = a_recv[s, 0:8, :]
        top = a_recv[s, 8:9, :]
        where_q = (top + ((fold8 - top) & 15)) >> 4
        for q in range(4):
            take = (where_q == q) & (depth < near[q])
            near[q] = jnp.where(take, depth, near[q])
            winner[q] = jnp.where(take, s, winner[q])

    def upper_half(top):
        return (top + ((fold16 - top) & 31)) >= 32

    def take_tops():
        pl.when(me_w != hub)(lambda: all_of(nw, t_recv, t_rs))
        for b in range(nw):
            mine = jnp.where(lax.broadcasted_iota(I32, (1, 128), 1) == me_w, t_recv[b], 0).astype(F32)
            tops_of[b] = jnp.broadcast_to(jnp.sum(mine, axis=1, keepdims=True), (1, 128)).astype(I32)

    def limit_copy(peer, src, rows):
        return pltpu.make_async_remote_copy(
            src_ref=src, dst_ref=l_recv.at[me_w, pl.ds(0, rows)], send_sem=l_ss, recv_sem=l_rs.at[me_w],
            device_id=(peer, me_g), device_id_type=MESH,
        )

    near_lo = jnp.concatenate(near[:2], axis=0)
    near_hi = jnp.concatenate(near[2:], axis=0)
    l_full[0:16, :] = near_lo
    l_full[16:32, :] = near_hi

    @pl.when(late)
    def _():
        l_recv[me_w] = l_full[...]
        pl.when(me_w != hub)(lambda: pl.semaphore_wait(w_ready, 1))
        for o in wide_offsets:
            limit_copy(wide_peer(o), l_full, LROWS).start()

    @pl.when(jnp.logical_not(late))
    def _():
        take_tops()
        for o in [*wide_offsets, (0, 0)]:
            l_send[wide_peer(o)] = jnp.where(upper_half(tops_of[wide_peer(o)]), l_full[16:32, :], l_full[0:16, :])
        l_recv[me_w, 0:16, :] = l_send[me_w]
        for o in wide_offsets:
            limit_copy(wide_peer(o), l_send.at[wide_peer(o)], 16).start()

    for o in grp_offsets:
        send_color(grp_peer(o), grp_peer(o) > me_g)
    pl.when((me_w == hub) & late)(pass_tops)

    def by_start():
        for k in range(nx + ny - 1):
            low, high = max(0, k - ny + 1), min(nx - 1, k)
            for i in range(high - low + 1):
                x = low + (me_w // ny + me_w % ny + i) % (high - low + 1)
                yield x * ny + k - x

    for c in by_start():
        for rows, here in ((LROWS, late), (16, jnp.logical_not(late))):
            part = l_recv.at[c, pl.ds(0, rows)]
            pl.when((me_w != c) & here)(lambda c=c, part=part: pltpu.make_async_copy(part, part, l_rs.at[c]).wait())
        limit = jnp.where(late & upper_half(vbox[0, c]), l_recv[c, 16:32, :], l_recv[c, 0:16, :])
        at = en[pl.ds(c * S, 16), :]
        stride = st[pl.ds(c * S, 16), :]
        word0 = jnp.zeros((16, 128), I32)
        word1 = jnp.zeros((16, 128), I32)
        for k in range(SAMPLES):
            kept = at < limit
            word0 = jnp.where(kept, tab0[c, k], word0)
            word1 = jnp.where(kept, tab1[c, k], word1)
            at = at + stride
        f_send[c, 0:16, :] = word0
        f_send[c, 16:32, :] = word1

        @pl.when(me_w != c)
        def _(c=c):
            wide_copy(c, f_send, f_recv, f_ss, f_rs).start()

    f_recv[me_w] = f_send[me_w]
    pl.when(late)(take_tops)
    all_of(ng - 1, c_recv, c_rs)
    color = [[jnp.zeros((8, 128), F32) for _ in range(3)] for _ in range(4)]
    for s in range(ng):
        rgb = [c_recv[s, ch].astype(F32) for ch in range(3)]
        for q in range(4):
            won = winner[q] == s
            color[q] = [jnp.where(won, rgb[ch], color[q][ch]) for ch in range(3)]
    for ch in range(3):
        for q in range(4):
            surf[ch, 8 * q : 8 * q + 8, :] = color[q][ch]

    all_of(nw - 1, f_recv, f_rs)
    through = [jnp.ones((16, 128), F32) for _ in range(2)]
    total = [[jnp.zeros((16, 128), F32) for _ in range(3)] for _ in range(2)]
    loads[3].wait()
    for j in range(nw):
        b = order[0, j]
        word0, word1 = f_recv[b, 0:16, :], f_recv[b, 16:32, :]
        upper = upper_half(tops_of[b])
        layer = [
            lax.shift_right_logical(word0, 16).astype(F32),
            (word0 & 65535).astype(F32),
            lax.shift_right_logical(word1, 16).astype(F32),
        ]
        opaque = (word1 & 65535).astype(F32) * (1.0 / ALPHA_SCALE)
        for h in range(2):
            weight = jnp.where(upper, through[h], 0.0) if h else jnp.where(upper, 0.0, through[h])
            total[h] = [total[h][ch] + weight * layer[ch] for ch in range(3)]
            through[h] = through[h] - weight * opaque
    for h in range(2):
        rows = slice(16 * h, 16 * h + 16)
        for ch in range(3):
            od[ch * S + 16 * h : ch * S + 16 * h + 16, :] = (
                total[h][ch] * (1.0 / COLOR_SCALE) + through[h] * surf[ch, rows, :]
            )
        od[3 * S + 16 * h : 3 * S + 16 * h + 16, :] = through[h]
    for j in range(LROWS):
        out[:, 128 * j : 128 * j + 128] = od[pl.ds(j, 4, stride=S), :]

    for n, buf, sem in (
        (ng - 1, a_send, a_ss), (ng - 1, c_send, c_ss), (nw - 1, f_send, f_ss),
    ):
        all_of(n, buf, sem)

    pl.when(late)(lambda: all_of(nw - 1, l_recv, l_ss))
    pl.when(jnp.logical_not(late))(lambda: all_of(nw - 1, l_send, l_ss))

    @pl.when(me_w != hub)
    def _():
        pltpu.make_async_copy(t_send, t_send, t_ss).wait()

    @pl.when(me_w == hub)
    def _():
        for o in wide_offsets:
            all_of(nw, t_recv, t_ss)


def per_device(dims, surf_depth, surf_color, surf_box, vol_color, vol_alpha, vol_box, ray_entry, ray_step, order):
    nx, ny, nz, ncore = dims
    nw, ng = nx * ny, nz * ncore
    V, D = pltpu.VMEM, pltpu.SemaphoreType.DMA
    bf16 = jnp.bfloat16
    hbm = pl.BlockSpec(memory_space=pltpu.HBM)
    frame = pl.pallas_call(
        functools.partial(kernel, dims),
        out_shape=pltpu.VMEM((4, PIX), F32),
        in_specs=[hbm] * 9,
        out_specs=pl.BlockSpec(memory_space=pltpu.VMEM),
        scratch_shapes=[
            pltpu.SMEM((4, ng), I32), pltpu.SMEM((4, nw), I32), pltpu.SMEM((1, nw), I32),
            V((ng, PIX), I32), V((3, ng, PIX), bf16), V((nw, 3, SAMPLES, PIX), bf16), V((nw, SAMPLES, PIX), bf16),
            V((nw, PIX), I32), V((nw, PIX), I32),
            V((ng * S, 128), I32), V((3, ng * S, 128), F32), V((nw * S, 128), I32), V((nw * S, 128), I32),
            V((SAMPLES * S, 128), F32), V((3, SAMPLES * S, 128), F32),
            V((ng, 9, 128), I32), V((ng, 9, 128), I32),
            V((ng, 3, 8, 128), bf16), V((ng, 3, 8, 128), bf16),
            V((1, 128), I32), V((nw, 1, 128), I32), V((nw, 1, 128), I32),
            V((LROWS, 128), I32), V((nw, 16, 128), I32), V((nw, LROWS, 128), I32),
            V((nw, LROWS, 128), I32), V((nw, LROWS, 128), I32),
            V((nw, SAMPLES, 16, 128), I32), V((nw, SAMPLES, 16, 128), I32),
            V((3, LROWS, 128), F32), V((4 * S, 128), F32),
            D((9,)), pltpu.SemaphoreType.REGULAR, pltpu.SemaphoreType.REGULAR,
            D, D((2,)), D, D, D, D, D, D((nw,)), D, D,
        ],
        compiler_params=pltpu.CompilerParams(
            collective_id=0, has_side_effects=True, vmem_limit_bytes=66977792
        ),
    )(
        surf_depth[0, 0],
        jnp.transpose(surf_color[0, 0], (1, 0, 2)),
        surf_box[0, 0].T,
        jnp.transpose(vol_color[0, 0], (0, 2, 1, 3)),
        vol_alpha[0, 0],
        vol_box[0, 0].T,
        ray_entry[0, 0],
        ray_step[0, 0],
        order,
    )
    return frame[None, None]


def solution(mesh):
    nw, ng = mesh.shape["wide"], mesh.shape["grp"]
    nx = max(d for d in range(1, nw + 1) if d * d <= nw and nw % d == 0)
    dims = (nx, nw // nx, ng // 2, 2)
    return jax.shard_map(
        functools.partial(per_device, dims),
        mesh=mesh,
        in_specs=(
            P("wide", "grp", None, None),
            P("wide", "grp", None, None, None),
            P("wide", "grp", None, None),
            P("wide", "grp", None, None, None, None),
            P("wide", "grp", None, None, None),
            P("wide", "grp", None, None),
            P("wide", "grp", None, None),
            P("wide", "grp", None, None),
            P("grp", None),
        ),
        out_specs=P("grp", "wide", None, None),
        check_vma=False,
    )
```

```python
import functools

import jax
import jax.numpy as jnp
from jax import lax
from jax.experimental import pallas as pl
from jax.experimental.pallas import tpu as pltpu
from jax.sharding import PartitionSpec as P

MESH = pl.DeviceIdType.MESH
FAR = 1073741824
PIX = 4096
LROWS = 32
S = 40
SAMPLES = 8
COLOR_SCALE = 59000.0
ALPHA_SCALE = 236000.0

I32 = jnp.int32
F32 = jnp.float32


def far_first(nx, ny):
    ring = lambda d, n: min(d, n - d)
    offsets = [(a, b) for a in range(nx) for b in range(ny) if (a, b) != (0, 0)]
    return sorted(offsets, key=lambda o: -(ring(o[0], nx) + ring(o[1], ny)))


def kernel(
    dims,
    sdepth, scolor, sbox_hbm, vcolor, valpha, vbox_hbm, entry, step, order_hbm,
    out,
    sbox, vbox, order,
    sd_nat, sc_nat, vc_nat, va_nat, en_nat, st_nat,
    sd, sc, en, st, ad, cd,
    a_send, a_recv, c_send, c_recv, t_send, t_hub, t_recv, tops_of, l_send, l_recv, f_send, f_recv,
    tab0, tab1, surf, od,
    lsem, g_ready, a_ss, a_rs, c_ss, c_rs, t_ss, h_rs, t_rs, l_ss, l_rs, f_ss, f_rs,
):
    nx, ny, nz, ncore = dims
    nw, ng = nx * ny, nz * ncore
    me_w, me_g = lax.axis_index("wide"), lax.axis_index("grp")
    wide_offsets, grp_offsets = far_first(nx, ny), far_first(nz, ncore)

    def wide_peer(o):
        x, y = me_w // ny, me_w % ny
        return ((x + o[0]) % nx) * ny + (y + o[1]) % ny

    def grp_peer(o):
        z, core = me_g // ncore, me_g % ncore
        return ((z + o[0]) % nz) * ncore + (core + o[1]) % ncore

    def wide_copy(peer, src, dst, ss, rs):
        return pltpu.make_async_remote_copy(
            src_ref=src.at[peer], dst_ref=dst.at[me_w], send_sem=ss, recv_sem=rs,
            device_id=(peer, me_g), device_id_type=MESH,
        )

    def grp_copy(peer, src, dst, ss, rs):
        return pltpu.make_async_remote_copy(
            src_ref=src.at[peer], dst_ref=dst.at[me_g], send_sem=ss, recv_sem=rs,
            device_id=(me_w, peer), device_id_type=MESH,
        )

    def all_of(n, buf, sem):
        pltpu.make_async_copy(buf.at[pl.ds(0, n)], buf.at[pl.ds(0, n)], sem).wait()

    half = ng // 2
    core = me_g % ncore
    first_g = me_g // ncore * ncore
    hub_g = first_g + ncore - 1
    is_hub = (me_w == 0) & (me_g == hub_g)
    barrier = pltpu.get_barrier_semaphore()

    def tell(sem, w, g):
        pl.semaphore_signal(sem, inc=1, device_id=(w, g), device_id_type=MESH)

    def tell_grp(sem, wants):
        for o in grp_offsets:
            peer = grp_peer(o)
            pl.when(wants(peer))(lambda peer=peer: tell(sem, me_w, peer))

    loads = []
    for i, (src, dst) in enumerate(
        (
            (sbox_hbm, sbox), (sdepth, sd_nat), (vbox_hbm, vbox), (order_hbm, order), (scolor, sc_nat),
            (valpha, va_nat), (vcolor, vc_nat), (entry, en_nat), (step, st_nat),
        )
    ):
        loads.append(pltpu.make_async_copy(src, dst, lsem.at[i]))
        if i < 4:
            loads[-1].start()
    tell_grp(barrier, lambda peer: peer > me_g)

    def planes(act):
        for k in range(ncore):
            for w in range(nw):
                if (k, w) != (ncore - 1, 0):
                    act(k, w)

    @pl.when(is_hub)
    def _():
        planes(lambda k, w: tell(barrier, w, first_g + k))

    for load in loads[4:]:
        load.start()

    def send_where(offsets, peer_of, me, copy, wants, *bufs):
        for o in offsets:
            pl.when(wants(peer_of(o), me))(lambda o=o: copy(peer_of(o), *bufs).start())

    lower, higher = (lambda peer, me: peer < me), (lambda peer, me: peer > me)

    row8 = lax.broadcasted_iota(I32, (8, 128), 0)
    lane8 = lax.broadcasted_iota(I32, (8, 128), 1)
    fold8 = 2 * row8 + (lane8 >> 6)
    col8 = lane8 & 63
    fold16 = 2 * lax.broadcasted_iota(I32, (16, 128), 0) + (lax.broadcasted_iota(I32, (16, 128), 1) >> 6)
    col16 = lax.broadcasted_iota(I32, (16, 128), 1) & 63

    def spread(nat, dense, n, lead=()):
        g = min(8, n)
        for h in range(n // g):
            for j in range(LROWS):
                tile = nat[(*lead, pl.ds(h * g, g), pl.ds(128 * j, 128))]
                if tile.dtype == jnp.bfloat16:
                    tile = tile.astype(F32)
                dense[pl.ds(h * g * S + j, g, stride=S), :] = tile

    loads[2].wait()
    tops = jnp.zeros((1, 128), I32)
    for c in range(nw):
        tops = jnp.where(lax.broadcasted_iota(I32, (1, 128), 1) == c, vbox[0, c], tops)
    t_send[...] = tops
    entered = me_g + jnp.logical_not(is_hub).astype(I32)
    pl.when(entered > 0)(lambda: pl.semaphore_wait(barrier, entered))
    tell_grp(g_ready, lambda peer: peer < me_g)

    for k in range(ncore):

        @pl.when((core == k) & jnp.logical_not(is_hub))
        def _(k=k):
            pltpu.make_async_remote_copy(
                src_ref=t_send, dst_ref=t_hub.at[k, me_w], send_sem=t_ss, recv_sem=h_rs.at[k],
                device_id=(0, hub_g), device_id_type=MESH,
            ).start()

    loads[0].wait()
    loads[1].wait()
    spread(sd_nat, sd, ng)

    def surface_inside(r):
        inx = (col8 >= sbox[2, r]) & (col8 < sbox[3, r])
        return [
            inx & (fold8 + 16 * q >= sbox[0, r]) & (fold8 + 16 * q < sbox[1, r]) for q in range(4)
        ]

    def send_depth(peer, wanted):
        pl.when(wanted)(lambda: grp_copy(peer, a_send, a_recv, a_ss, a_rs.at[me_g // half]).start())

    def send_color(peer, wanted):
        pl.when(wanted)(lambda: grp_copy(peer, c_send, c_recv, c_ss, c_rs).start())

    for r in range(ng):
        folded = jnp.full((8, 128), FAR, I32)
        for q, inside in enumerate(surface_inside(r)):
            folded = jnp.where(inside, sd[pl.ds(r * S + 8 * q, 8), :], folded)
        a_send[r, 0:8, :] = folded
        a_send[r, 8:9, :] = jnp.full((1, 128), sbox[0, r], I32)
        if r:
            send_depth(r - 1, r - 1 < me_g)
    a_recv[me_g] = a_send[me_g]

    loads[4].wait()
    for ch in range(3):
        spread(sc_nat, sc.at[ch], ng, (ch,))

    def fold_color(r, carry):
        inside = surface_inside(r)
        for ch in range(3):
            folded = jnp.zeros((8, 128), F32)
            for q in range(4):
                folded = jnp.where(inside[q], sc[ch, pl.ds(r * S + 8 * q, 8), :], folded)
            c_send[r, ch] = folded.astype(jnp.bfloat16)
        return carry

    lax.fori_loop(0, ng, fold_color, 0)
    c_recv[me_g] = c_send[me_g]

    for load in loads[5:]:
        load.wait()
    spread(en_nat, en, nw)
    spread(st_nat, st, nw)

    lane1 = lax.broadcasted_iota(I32, (8, 128), 1) >> 6

    def prefixes(c, carry):
        top, bottom = vbox[0, c], vbox[1, c]
        for j in range(16):
            s = lane1 + 2 * j
            upper = (top + ((s - top) & 31)) >= 32
            px, px2 = pl.ds(128 * j, 128), pl.ds(128 * (j + 16), 128)
            ad[pl.ds(j, SAMPLES, stride=S), :] = jnp.where(
                upper, va_nat[c, :, px2].astype(F32), va_nat[c, :, px].astype(F32)
            )
            for ch in range(3):
                cd[ch, pl.ds(j, SAMPLES, stride=S), :] = jnp.where(
                    upper, vc_nat[c, ch, :, px2].astype(F32), vc_nat[c, ch, :, px].astype(F32)
                )
        y = top + ((fold16 - top) & 31)
        upper = y >= 32
        inside = (y < bottom) & (col16 >= vbox[2, c]) & (col16 < vbox[3, c])
        first = jnp.where(upper, en[pl.ds(c * S + 16, 16), :], en[pl.ds(c * S, 16), :])
        en[pl.ds(c * S, 16), :] = jnp.where(inside, first, FAR)
        st[pl.ds(c * S, 16), :] = jnp.where(upper, st[pl.ds(c * S + 16, 16), :], st[pl.ds(c * S, 16), :])
        trans = jnp.ones((16, 128), F32)
        accum = [jnp.zeros((16, 128), F32) for _ in range(3)]
        for k in range(SAMPLES):
            alpha = ad[pl.ds(k * S, 16), :]
            weight = trans * alpha
            trans = trans * (1.0 - alpha)
            for ch in range(3):
                accum[ch] = accum[ch] + weight * cd[ch, pl.ds(k * S, 16), :]
            r, g, b = [(a * COLOR_SCALE + 0.5).astype(I32) for a in accum]
            t = ((1.0 - trans) * ALPHA_SCALE + 0.5).astype(I32)
            tab0[c, k] = (r << 16) | g
            tab1[c, k] = (b << 16) | t
        return carry

    lax.fori_loop(0, nw, prefixes, 0)

    def pass_tops():
        for k in reversed(range(ncore)):
            all_of(nw - 1 if k == ncore - 1 else nw, t_hub.at[k], h_rs.at[k])
            if k == ncore - 1:
                t_hub[k, 0] = t_send[...]
                t_recv[...] = t_hub[k]
            for w in range(nw):
                if (k, w) != (ncore - 1, 0):
                    pltpu.make_async_remote_copy(
                        src_ref=t_hub.at[k], dst_ref=t_recv, send_sem=t_ss, recv_sem=t_rs,
                        device_id=(w, first_g + k), device_id_type=MESH,
                    ).start()

    pl.when(is_hub & (me_g < ncore))(pass_tops)
    for o in grp_offsets:
        send_color(grp_peer(o), grp_peer(o) < me_g)
    pl.when(me_g < ng - 1)(lambda: pl.semaphore_wait(g_ready, ng - 1 - me_g))
    for o in grp_offsets:
        send_depth(grp_peer(o), grp_peer(o) > me_g)

    pl.when(is_hub & (me_g >= ncore))(pass_tops)

    near = [jnp.full((8, 128), FAR, I32) for _ in range(4)]
    winner = [jnp.full((8, 128), -1, I32) for _ in range(4)]
    for s in range(ng):
        if s % half == 0:
            own = me_g // half == s // half
            pl.when(own)(lambda: all_of(half - 1, a_recv, a_rs.at[s // half]))
            pl.when(jnp.logical_not(own))(lambda: all_of(half, a_recv, a_rs.at[s // half]))
        depth = a_recv[s, 0:8, :]
        top = a_recv[s, 8:9, :]
        where_q = (top + ((fold8 - top) & 15)) >> 4
        for q in range(4):
            take = (where_q == q) & (depth < near[q])
            near[q] = jnp.where(take, depth, near[q])
            winner[q] = jnp.where(take, s, winner[q])

    def upper_half(top):
        return (top + ((fold16 - top) & 31)) >= 32

    near_lo = jnp.concatenate(near[:2], axis=0)
    near_hi = jnp.concatenate(near[2:], axis=0)
    pl.when(jnp.logical_not(is_hub))(lambda: all_of(nw, t_recv, t_rs))
    for b in range(nw):
        mine = jnp.where(lax.broadcasted_iota(I32, (1, 128), 1) == me_w, t_recv[b], 0).astype(F32)
        tops_of[b] = jnp.broadcast_to(jnp.sum(mine, axis=1, keepdims=True), (1, 128)).astype(I32)
    for o in [*wide_offsets, (0, 0)]:
        l_send[wide_peer(o)] = jnp.where(upper_half(tops_of[wide_peer(o)]), near_hi, near_lo)
    l_recv[me_w] = l_send[me_w]
    for o in wide_offsets:
        wide_copy(wide_peer(o), l_send, l_recv, l_ss, l_rs.at[me_w]).start()
    for o in grp_offsets:
        send_color(grp_peer(o), grp_peer(o) > me_g)

    def by_start():
        for k in range(nx + ny - 1):
            low, high = max(0, k - ny + 1), min(nx - 1, k)
            for i in range(high - low + 1):
                x = low + (me_w // ny + me_w % ny + i) % (high - low + 1)
                yield x * ny + k - x

    for c in by_start():
        pl.when(me_w != c)(lambda c=c: pltpu.make_async_copy(l_recv.at[c], l_recv.at[c], l_rs.at[c]).wait())
        limit = l_recv[c]
        at = en[pl.ds(c * S, 16), :]
        stride = st[pl.ds(c * S, 16), :]
        word0 = jnp.zeros((16, 128), I32)
        word1 = jnp.zeros((16, 128), I32)
        for k in range(SAMPLES):
            kept = at < limit
            word0 = jnp.where(kept, tab0[c, k], word0)
            word1 = jnp.where(kept, tab1[c, k], word1)
            at = at + stride
        f_send[c, 0:16, :] = word0
        f_send[c, 16:32, :] = word1

        @pl.when(me_w != c)
        def _(c=c):
            wide_copy(c, f_send, f_recv, f_ss, f_rs).start()

    f_recv[me_w] = f_send[me_w]
    all_of(ng - 1, c_recv, c_rs)
    color = [[jnp.zeros((8, 128), F32) for _ in range(3)] for _ in range(4)]
    for s in range(ng):
        rgb = [c_recv[s, ch].astype(F32) for ch in range(3)]
        for q in range(4):
            won = winner[q] == s
            color[q] = [jnp.where(won, rgb[ch], color[q][ch]) for ch in range(3)]
    for ch in range(3):
        for q in range(4):
            surf[ch, 8 * q : 8 * q + 8, :] = color[q][ch]

    all_of(nw - 1, f_recv, f_rs)
    through = [jnp.ones((16, 128), F32) for _ in range(2)]
    total = [[jnp.zeros((16, 128), F32) for _ in range(3)] for _ in range(2)]
    loads[3].wait()
    for j in range(nw):
        b = order[0, j]
        word0, word1 = f_recv[b, 0:16, :], f_recv[b, 16:32, :]
        upper = upper_half(tops_of[b])
        layer = [
            lax.shift_right_logical(word0, 16).astype(F32),
            (word0 & 65535).astype(F32),
            lax.shift_right_logical(word1, 16).astype(F32),
        ]
        opaque = (word1 & 65535).astype(F32) * (1.0 / ALPHA_SCALE)
        for h in range(2):
            weight = jnp.where(upper, through[h], 0.0) if h else jnp.where(upper, 0.0, through[h])
            total[h] = [total[h][ch] + weight * layer[ch] for ch in range(3)]
            through[h] = through[h] - weight * opaque
    for h in range(2):
        rows = slice(16 * h, 16 * h + 16)
        for ch in range(3):
            od[ch * S + 16 * h : ch * S + 16 * h + 16, :] = (
                total[h][ch] * (1.0 / COLOR_SCALE) + through[h] * surf[ch, rows, :]
            )
        od[3 * S + 16 * h : 3 * S + 16 * h + 16, :] = through[h]
    for j in range(LROWS):
        out[:, 128 * j : 128 * j + 128] = od[pl.ds(j, 4, stride=S), :]

    for n, buf, sem in (
        (ng - 1, a_send, a_ss), (ng - 1, c_send, c_ss), (nw - 1, l_send, l_ss), (nw - 1, f_send, f_ss),
    ):
        all_of(n, buf, sem)

    pl.when(jnp.logical_not(is_hub))(lambda: pltpu.make_async_copy(t_send, t_send, t_ss).wait())

    @pl.when(is_hub)
    def _():
        planes(lambda k, w: all_of(nw, t_recv, t_ss))


def per_device(dims, surf_depth, surf_color, surf_box, vol_color, vol_alpha, vol_box, ray_entry, ray_step, order):
    nx, ny, nz, ncore = dims
    nw, ng = nx * ny, nz * ncore
    V, D = pltpu.VMEM, pltpu.SemaphoreType.DMA
    bf16 = jnp.bfloat16
    hbm = pl.BlockSpec(memory_space=pltpu.HBM)
    frame = pl.pallas_call(
        functools.partial(kernel, dims),
        out_shape=pltpu.VMEM((4, PIX), F32),
        in_specs=[hbm] * 9,
        out_specs=pl.BlockSpec(memory_space=pltpu.VMEM),
        scratch_shapes=[
            pltpu.SMEM((4, ng), I32), pltpu.SMEM((4, nw), I32), pltpu.SMEM((1, nw), I32),
            V((ng, PIX), I32), V((3, ng, PIX), bf16), V((nw, 3, SAMPLES, PIX), bf16), V((nw, SAMPLES, PIX), bf16),
            V((nw, PIX), I32), V((nw, PIX), I32),
            V((ng * S, 128), I32), V((3, ng * S, 128), F32), V((nw * S, 128), I32), V((nw * S, 128), I32),
            V((SAMPLES * S, 128), F32), V((3, SAMPLES * S, 128), F32),
            V((ng, 9, 128), I32), V((ng, 9, 128), I32),
            V((ng, 3, 8, 128), bf16), V((ng, 3, 8, 128), bf16),
            V((1, 128), I32), V((ncore, nw, 1, 128), I32), V((nw, 1, 128), I32), V((nw, 1, 128), I32),
            V((nw, 16, 128), I32), V((nw, 16, 128), I32),
            V((nw, LROWS, 128), I32), V((nw, LROWS, 128), I32),
            V((nw, SAMPLES, 16, 128), I32), V((nw, SAMPLES, 16, 128), I32),
            V((3, LROWS, 128), F32), V((4 * S, 128), F32),
            D((9,)), pltpu.SemaphoreType.REGULAR,
            D, D((2,)), D, D, D, D((ncore,)), D, D, D((nw,)), D, D,
        ],
        compiler_params=pltpu.CompilerParams(
            collective_id=0, has_side_effects=True, vmem_limit_bytes=66977792
        ),
    )(
        surf_depth[0, 0],
        jnp.transpose(surf_color[0, 0], (1, 0, 2)),
        surf_box[0, 0].T,
        jnp.transpose(vol_color[0, 0], (0, 2, 1, 3)),
        vol_alpha[0, 0],
        vol_box[0, 0].T,
        ray_entry[0, 0],
        ray_step[0, 0],
        order,
    )
    return frame[None, None]


def solution(mesh):
    nw, ng = mesh.shape["wide"], mesh.shape["grp"]
    nx = max(d for d in range(1, nw + 1) if d * d <= nw and nw % d == 0)
    dims = (nx, nw // nx, ng // 2, 2)
    return jax.shard_map(
        functools.partial(per_device, dims),
        mesh=mesh,
        in_specs=(
            P("wide", "grp", None, None),
            P("wide", "grp", None, None, None),
            P("wide", "grp", None, None),
            P("wide", "grp", None, None, None, None),
            P("wide", "grp", None, None, None),
            P("wide", "grp", None, None),
            P("wide", "grp", None, None),
            P("wide", "grp", None, None),
            P("grp", None),
        ),
        out_specs=P("grp", "wide", None, None),
        check_vma=False,
    )
```

```python
import functools

import jax
import jax.numpy as jnp
from jax import lax
from jax.experimental import pallas as pl
from jax.experimental.pallas import tpu as pltpu
from jax.sharding import PartitionSpec as P

MESH = pl.DeviceIdType.MESH
FAR = 1073741824
PIX = 4096
LROWS = 32
S = 40
SAMPLES = 8
COLOR_SCALE = 59000.0
ALPHA_SCALE = 236000.0

I32 = jnp.int32
F32 = jnp.float32


def far_first(nx, ny):
    ring = lambda d, n: min(d, n - d)
    offsets = [(a, b) for a in range(nx) for b in range(ny) if (a, b) != (0, 0)]
    return sorted(offsets, key=lambda o: -(ring(o[0], nx) + ring(o[1], ny)))


def kernel(
    dims,
    sdepth, scolor, sbox_hbm, vcolor, valpha, vbox_hbm, entry, step, order_hbm,
    out,
    sbox, vbox, order,
    sd_nat, sc_nat, vc_nat, va_nat, en_nat, st_nat,
    sd, sc, en, st, ad, cd,
    a_send, a_recv, c_send, c_recv, t_send, t_hub, t_recv, tops_of, l_send, l_recv, f_send, f_recv,
    tab0, tab1, surf, od,
    lsem, g_ready, a_ss, a_rs, c_ss, c_rs, t_ss, h_rs, t_rs, l_ss, l_rs, f_ss, f_rs,
):
    nx, ny, nz, ncore = dims
    nw, ng = nx * ny, nz * ncore
    me_w, me_g = lax.axis_index("wide"), lax.axis_index("grp")
    wide_offsets, grp_offsets = far_first(nx, ny), far_first(nz, ncore)

    def wide_peer(o):
        x, y = me_w // ny, me_w % ny
        return ((x + o[0]) % nx) * ny + (y + o[1]) % ny

    def grp_peer(o):
        z, core = me_g // ncore, me_g % ncore
        return ((z + o[0]) % nz) * ncore + (core + o[1]) % ncore

    def wide_copy(peer, src, dst, ss, rs):
        return pltpu.make_async_remote_copy(
            src_ref=src.at[peer], dst_ref=dst.at[me_w], send_sem=ss, recv_sem=rs,
            device_id=(peer, me_g), device_id_type=MESH,
        )

    def grp_copy(peer, src, dst, ss, rs):
        return pltpu.make_async_remote_copy(
            src_ref=src.at[peer], dst_ref=dst.at[me_g], send_sem=ss, recv_sem=rs,
            device_id=(me_w, peer), device_id_type=MESH,
        )

    def all_of(n, buf, sem):
        pltpu.make_async_copy(buf.at[pl.ds(0, n)], buf.at[pl.ds(0, n)], sem).wait()

    half = ng // 2
    core = me_g % ncore
    first_g = me_g // ncore * ncore
    hub_g = first_g + ncore - 1
    is_hub = (me_w == 0) & (me_g == hub_g)
    barrier = pltpu.get_barrier_semaphore()

    def tell(sem, w, g):
        pl.semaphore_signal(sem, inc=1, device_id=(w, g), device_id_type=MESH)

    def tell_grp(sem, wants):
        for o in grp_offsets:
            peer = grp_peer(o)
            pl.when(wants(peer))(lambda peer=peer: tell(sem, me_w, peer))

    loads = []
    for i, (src, dst) in enumerate(
        (
            (sbox_hbm, sbox), (sdepth, sd_nat), (vbox_hbm, vbox), (order_hbm, order), (scolor, sc_nat),
            (valpha, va_nat), (vcolor, vc_nat), (entry, en_nat), (step, st_nat),
        )
    ):
        loads.append(pltpu.make_async_copy(src, dst, lsem.at[i]))
        if i < 4:
            loads[-1].start()
    tell_grp(barrier, lambda peer: peer > me_g)

    def planes(act):
        for k in range(ncore):
            for w in range(nw):
                if (k, w) != (ncore - 1, 0):
                    act(k, w)

    @pl.when(is_hub)
    def _():
        planes(lambda k, w: tell(barrier, w, first_g + k))

    for load in loads[4:]:
        load.start()

    def send_where(offsets, peer_of, me, copy, wants, *bufs):
        for o in offsets:
            pl.when(wants(peer_of(o), me))(lambda o=o: copy(peer_of(o), *bufs).start())

    lower, higher = (lambda peer, me: peer < me), (lambda peer, me: peer > me)

    row8 = lax.broadcasted_iota(I32, (8, 128), 0)
    lane8 = lax.broadcasted_iota(I32, (8, 128), 1)
    fold8 = 2 * row8 + (lane8 >> 6)
    col8 = lane8 & 63
    fold16 = 2 * lax.broadcasted_iota(I32, (16, 128), 0) + (lax.broadcasted_iota(I32, (16, 128), 1) >> 6)
    col16 = lax.broadcasted_iota(I32, (16, 128), 1) & 63

    def spread(nat, dense, n, lead=()):
        g = min(8, n)
        for h in range(n // g):
            for j in range(LROWS):
                tile = nat[(*lead, pl.ds(h * g, g), pl.ds(128 * j, 128))]
                if tile.dtype == jnp.bfloat16:
                    tile = tile.astype(F32)
                dense[pl.ds(h * g * S + j, g, stride=S), :] = tile

    loads[2].wait()
    tops = jnp.zeros((1, 128), I32)
    for c in range(nw):
        tops = jnp.where(lax.broadcasted_iota(I32, (1, 128), 1) == c, vbox[0, c], tops)
    t_send[...] = tops
    entered = me_g + jnp.logical_not(is_hub).astype(I32)
    pl.when(entered > 0)(lambda: pl.semaphore_wait(barrier, entered))
    tell_grp(g_ready, lambda peer: peer < me_g)

    for k in range(ncore):

        @pl.when((core == k) & jnp.logical_not(is_hub))
        def _(k=k):
            pltpu.make_async_remote_copy(
                src_ref=t_send, dst_ref=t_hub.at[k, me_w], send_sem=t_ss, recv_sem=h_rs.at[k],
                device_id=(0, hub_g), device_id_type=MESH,
            ).start()

    loads[0].wait()
    loads[1].wait()
    spread(sd_nat, sd, ng)

    def surface_inside(r):
        inx = (col8 >= sbox[2, r]) & (col8 < sbox[3, r])
        return [
            inx & (fold8 + 16 * q >= sbox[0, r]) & (fold8 + 16 * q < sbox[1, r]) for q in range(4)
        ]

    def send_depth(peer, wanted):
        pl.when(wanted)(lambda: grp_copy(peer, a_send, a_recv, a_ss, a_rs.at[me_g // half]).start())

    def send_color(peer, wanted):
        pl.when(wanted)(lambda: grp_copy(peer, c_send, c_recv, c_ss, c_rs).start())

    for r in range(ng):
        folded = jnp.full((8, 128), FAR, I32)
        for q, inside in enumerate(surface_inside(r)):
            folded = jnp.where(inside, sd[pl.ds(r * S + 8 * q, 8), :], folded)
        a_send[r, 0:8, :] = folded
        a_send[r, 8:9, :] = jnp.full((1, 128), sbox[0, r], I32)
        if r:
            send_depth(r - 1, r - 1 < me_g)
    a_recv[me_g] = a_send[me_g]

    loads[4].wait()
    for ch in range(3):
        spread(sc_nat, sc.at[ch], ng, (ch,))

    def fold_color(r, carry):
        inside = surface_inside(r)
        for ch in range(3):
            folded = jnp.zeros((8, 128), F32)
            for q in range(4):
                folded = jnp.where(inside[q], sc[ch, pl.ds(r * S + 8 * q, 8), :], folded)
            c_send[r, ch] = folded.astype(jnp.bfloat16)
        return carry

    lax.fori_loop(0, ng, fold_color, 0)
    c_recv[me_g] = c_send[me_g]

    for load in loads[5:]:
        load.wait()
    spread(en_nat, en, nw)
    spread(st_nat, st, nw)

    lane1 = lax.broadcasted_iota(I32, (8, 128), 1) >> 6

    def prefixes(c, carry):
        top, bottom = vbox[0, c], vbox[1, c]
        for j in range(16):
            s = lane1 + 2 * j
            upper = (top + ((s - top) & 31)) >= 32
            px, px2 = pl.ds(128 * j, 128), pl.ds(128 * (j + 16), 128)
            ad[pl.ds(j, SAMPLES, stride=S), :] = jnp.where(
                upper, va_nat[c, :, px2].astype(F32), va_nat[c, :, px].astype(F32)
            )
            for ch in range(3):
                cd[ch, pl.ds(j, SAMPLES, stride=S), :] = jnp.where(
                    upper, vc_nat[c, ch, :, px2].astype(F32), vc_nat[c, ch, :, px].astype(F32)
                )
        y = top + ((fold16 - top) & 31)
        upper = y >= 32
        inside = (y < bottom) & (col16 >= vbox[2, c]) & (col16 < vbox[3, c])
        first = jnp.where(upper, en[pl.ds(c * S + 16, 16), :], en[pl.ds(c * S, 16), :])
        en[pl.ds(c * S, 16), :] = jnp.where(inside, first, FAR)
        st[pl.ds(c * S, 16), :] = jnp.where(upper, st[pl.ds(c * S + 16, 16), :], st[pl.ds(c * S, 16), :])
        trans = jnp.ones((16, 128), F32)
        accum = [jnp.zeros((16, 128), F32) for _ in range(3)]
        for k in range(SAMPLES):
            alpha = ad[pl.ds(k * S, 16), :]
            weight = trans * alpha
            trans = trans * (1.0 - alpha)
            for ch in range(3):
                accum[ch] = accum[ch] + weight * cd[ch, pl.ds(k * S, 16), :]
            r, g, b = [(a * COLOR_SCALE + 0.5).astype(I32) for a in accum]
            t = ((1.0 - trans) * ALPHA_SCALE + 0.5).astype(I32)
            tab0[c, k] = (r << 16) | g
            tab1[c, k] = (b << 16) | t
        return carry

    lax.fori_loop(0, nw, prefixes, 0)

    def pass_tops():
        for k in reversed(range(ncore)):
            all_of(nw - 1 if k == ncore - 1 else nw, t_hub.at[k], h_rs.at[k])
            if k == ncore - 1:
                t_hub[k, 0] = t_send[...]
                t_recv[...] = t_hub[k]
            for w in range(nw):
                if (k, w) != (ncore - 1, 0):
                    pltpu.make_async_remote_copy(
                        src_ref=t_hub.at[k], dst_ref=t_recv, send_sem=t_ss, recv_sem=t_rs,
                        device_id=(w, first_g + k), device_id_type=MESH,
                    ).start()

    pl.when(is_hub & (me_g < ncore))(pass_tops)
    for o in grp_offsets:
        send_color(grp_peer(o), grp_peer(o) < me_g)
    pl.when(me_g < ng - 1)(lambda: pl.semaphore_wait(g_ready, ng - 1 - me_g))
    for o in grp_offsets:
        send_depth(grp_peer(o), grp_peer(o) > me_g)

    pl.when(is_hub & (me_g >= ncore))(pass_tops)

    def take_tops():
        pl.when(jnp.logical_not(is_hub))(lambda: all_of(nw, t_recv, t_rs))
        for b in range(nw):
            mine = jnp.where(lax.broadcasted_iota(I32, (1, 128), 1) == me_w, t_recv[b], 0).astype(F32)
            tops_of[b] = jnp.broadcast_to(jnp.sum(mine, axis=1, keepdims=True), (1, 128)).astype(I32)

    near = [jnp.full((8, 128), FAR, I32) for _ in range(4)]
    winner = [jnp.full((8, 128), -1, I32) for _ in range(4)]
    for s in range(ng):
        if s == half:
            take_tops()
        if s % half == 0:
            own = me_g // half == s // half
            pl.when(own)(lambda: all_of(half - 1, a_recv, a_rs.at[s // half]))
            pl.when(jnp.logical_not(own))(lambda: all_of(half, a_recv, a_rs.at[s // half]))
        depth = a_recv[s, 0:8, :]
        top = a_recv[s, 8:9, :]
        where_q = (top + ((fold8 - top) & 15)) >> 4
        for q in range(4):
            take = (where_q == q) & (depth < near[q])
            near[q] = jnp.where(take, depth, near[q])
            winner[q] = jnp.where(take, s, winner[q])

    def upper_half(top):
        return (top + ((fold16 - top) & 31)) >= 32

    near_lo = jnp.concatenate(near[:2], axis=0)
    near_hi = jnp.concatenate(near[2:], axis=0)
    for o in [*wide_offsets, (0, 0)]:
        l_send[wide_peer(o)] = jnp.where(upper_half(tops_of[wide_peer(o)]), near_hi, near_lo)
    l_recv[me_w] = l_send[me_w]
    for o in wide_offsets:
        wide_copy(wide_peer(o), l_send, l_recv, l_ss, l_rs.at[me_w]).start()
    for o in grp_offsets:
        send_color(grp_peer(o), grp_peer(o) > me_g)

    def by_start():
        for k in range(nx + ny - 1):
            low, high = max(0, k - ny + 1), min(nx - 1, k)
            for i in range(high - low + 1):
                x = low + (me_w // ny + me_w % ny + i) % (high - low + 1)
                yield x * ny + k - x

    for c in by_start():
        pl.when(me_w != c)(lambda c=c: pltpu.make_async_copy(l_recv.at[c], l_recv.at[c], l_rs.at[c]).wait())
        limit = l_recv[c]
        at = en[pl.ds(c * S, 16), :]
        stride = st[pl.ds(c * S, 16), :]
        word0 = jnp.zeros((16, 128), I32)
        word1 = jnp.zeros((16, 128), I32)
        for k in range(SAMPLES):
            kept = at < limit
            word0 = jnp.where(kept, tab0[c, k], word0)
            word1 = jnp.where(kept, tab1[c, k], word1)
            at = at + stride
        f_send[c, 0:16, :] = word0
        f_send[c, 16:32, :] = word1

        @pl.when(me_w != c)
        def _(c=c):
            wide_copy(c, f_send, f_recv, f_ss, f_rs).start()

    f_recv[me_w] = f_send[me_w]
    all_of(ng - 1, c_recv, c_rs)
    color = [[jnp.zeros((8, 128), F32) for _ in range(3)] for _ in range(4)]
    for s in range(ng):
        rgb = [c_recv[s, ch].astype(F32) for ch in range(3)]
        for q in range(4):
            won = winner[q] == s
            color[q] = [jnp.where(won, rgb[ch], color[q][ch]) for ch in range(3)]
    for ch in range(3):
        for q in range(4):
            surf[ch, 8 * q : 8 * q + 8, :] = color[q][ch]

    all_of(nw - 1, f_recv, f_rs)
    through = [jnp.ones((16, 128), F32) for _ in range(2)]
    total = [[jnp.zeros((16, 128), F32) for _ in range(3)] for _ in range(2)]
    loads[3].wait()
    for j in range(nw):
        b = order[0, j]
        word0, word1 = f_recv[b, 0:16, :], f_recv[b, 16:32, :]
        upper = upper_half(tops_of[b])
        layer = [
            lax.shift_right_logical(word0, 16).astype(F32),
            (word0 & 65535).astype(F32),
            lax.shift_right_logical(word1, 16).astype(F32),
        ]
        opaque = (word1 & 65535).astype(F32) * (1.0 / ALPHA_SCALE)
        for h in range(2):
            weight = jnp.where(upper, through[h], 0.0) if h else jnp.where(upper, 0.0, through[h])
            total[h] = [total[h][ch] + weight * layer[ch] for ch in range(3)]
            through[h] = through[h] - weight * opaque
    for h in range(2):
        rows = slice(16 * h, 16 * h + 16)
        for ch in range(3):
            od[ch * S + 16 * h : ch * S + 16 * h + 16, :] = (
                total[h][ch] * (1.0 / COLOR_SCALE) + through[h] * surf[ch, rows, :]
            )
        od[3 * S + 16 * h : 3 * S + 16 * h + 16, :] = through[h]
    for j in range(LROWS):
        out[:, 128 * j : 128 * j + 128] = od[pl.ds(j, 4, stride=S), :]

    for n, buf, sem in (
        (ng - 1, a_send, a_ss), (ng - 1, c_send, c_ss), (nw - 1, l_send, l_ss), (nw - 1, f_send, f_ss),
    ):
        all_of(n, buf, sem)

    pl.when(jnp.logical_not(is_hub))(lambda: pltpu.make_async_copy(t_send, t_send, t_ss).wait())

    @pl.when(is_hub)
    def _():
        planes(lambda k, w: all_of(nw, t_recv, t_ss))


def per_device(dims, surf_depth, surf_color, surf_box, vol_color, vol_alpha, vol_box, ray_entry, ray_step, order):
    nx, ny, nz, ncore = dims
    nw, ng = nx * ny, nz * ncore
    V, D = pltpu.VMEM, pltpu.SemaphoreType.DMA
    bf16 = jnp.bfloat16
    hbm = pl.BlockSpec(memory_space=pltpu.HBM)
    frame = pl.pallas_call(
        functools.partial(kernel, dims),
        out_shape=pltpu.VMEM((4, PIX), F32),
        in_specs=[hbm] * 9,
        out_specs=pl.BlockSpec(memory_space=pltpu.VMEM),
        scratch_shapes=[
            pltpu.SMEM((4, ng), I32), pltpu.SMEM((4, nw), I32), pltpu.SMEM((1, nw), I32),
            V((ng, PIX), I32), V((3, ng, PIX), bf16), V((nw, 3, SAMPLES, PIX), bf16), V((nw, SAMPLES, PIX), bf16),
            V((nw, PIX), I32), V((nw, PIX), I32),
            V((ng * S, 128), I32), V((3, ng * S, 128), F32), V((nw * S, 128), I32), V((nw * S, 128), I32),
            V((SAMPLES * S, 128), F32), V((3, SAMPLES * S, 128), F32),
            V((ng, 9, 128), I32), V((ng, 9, 128), I32),
            V((ng, 3, 8, 128), bf16), V((ng, 3, 8, 128), bf16),
            V((1, 128), I32), V((ncore, nw, 1, 128), I32), V((nw, 1, 128), I32), V((nw, 1, 128), I32),
            V((nw, 16, 128), I32), V((nw, 16, 128), I32),
            V((nw, LROWS, 128), I32), V((nw, LROWS, 128), I32),
            V((nw, SAMPLES, 16, 128), I32), V((nw, SAMPLES, 16, 128), I32),
            V((3, LROWS, 128), F32), V((4 * S, 128), F32),
            D((9,)), pltpu.SemaphoreType.REGULAR,
            D, D((2,)), D, D, D, D((ncore,)), D, D, D((nw,)), D, D,
        ],
        compiler_params=pltpu.CompilerParams(
            collective_id=0, has_side_effects=True, vmem_limit_bytes=66977792
        ),
    )(
        surf_depth[0, 0],
        jnp.transpose(surf_color[0, 0], (1, 0, 2)),
        surf_box[0, 0].T,
        jnp.transpose(vol_color[0, 0], (0, 2, 1, 3)),
        vol_alpha[0, 0],
        vol_box[0, 0].T,
        ray_entry[0, 0],
        ray_step[0, 0],
        order,
    )
    return frame[None, None]


def solution(mesh):
    nw, ng = mesh.shape["wide"], mesh.shape["grp"]
    nx = max(d for d in range(1, nw + 1) if d * d <= nw and nw % d == 0)
    dims = (nx, nw // nx, ng // 2, 2)
    return jax.shard_map(
        functools.partial(per_device, dims),
        mesh=mesh,
        in_specs=(
            P("wide", "grp", None, None),
            P("wide", "grp", None, None, None),
            P("wide", "grp", None, None),
            P("wide", "grp", None, None, None, None),
            P("wide", "grp", None, None, None),
            P("wide", "grp", None, None),
            P("wide", "grp", None, None),
            P("wide", "grp", None, None),
            P("grp", None),
        ),
        out_specs=P("grp", "wide", None, None),
        check_vma=False,
    )
```
